1024 devices in a mesh: ctx: 32 (over z, core), exp: 32 (over y, x).
Axes of the slice: x: 4, y: 8, z: 16, core: 2. Of those that a mesh axis runs over, the one named last changes fastest.
Arguments:
- seq_inputs: bfloat16 [16384, 8192], P('ctx', 'exp'), may hold values from -6 to 6
- step_size: float32 [128, 16384], P('exp', 'ctx'), may hold values from 0.0007 to 0.14
- write_map: bfloat16 [16, 16384], P(None, 'ctx'), may hold values from -2 to 2
- read_map: bfloat16 [16, 16384], P(None, 'ctx'), may hold values from -2 to 2
- decay_log: float32 [128], P('exp'), may hold values from -9.3 to 1.4
- skip_gain: float32 [128], P('exp'), may hold values from 0.5 to 1.5
- moe_tokens: bfloat16 [4096, 4096], P('exp'), may hold values from -6 to 6
- expert_ids: int32 [4096, 2], P('exp'), may hold values from 0 to 15, all different within a row; in each aligned block of 128 rows (0 to 127, 128 to 255, ...) at most 32 rows name the same one
- route_weights: float32 [4096, 2], P('exp'), may hold values from 0.1 to 1
- gate_proj: bfloat16 [32, 4096, 3584], P('exp', None, 'ctx'), may hold values from -0.09375 to 0.09375
- up_proj: bfloat16 [32, 4096, 3584], P('exp', None, 'ctx'), may hold values from -0.09375 to 0.09375
- down_proj: bfloat16 [32, 3584, 4096], P('exp', None, 'ctx'), may hold values from -0.0625 to 0.0625
Outputs:
- mixer_output: bfloat16 [16384, 8192], P('ctx', 'exp')
- expert_output: bfloat16 [4096, 4096], P('exp', 'ctx')
The draws below stay inside these ranges and needn't reach their ends.
Inputs may be any that keep to these rules, and one draw needn't show every extreme that they name: `expert_ids`: each row names two different experts. In the 128 rows of one index of exp (aligned blocks), no expert is named more than 32 times, and in some blocks an expert is named exactly 32 times.
All inputs are finite; a program needn't handle non-finite values.
Results may differ from the reference program's by a relative error of at most 0.002.
The reference program's roundings to bfloat16 on the way count: a program that leaves them out, or rounds other values in their place, can miss the bound.
Values may be sent and summed in bfloat16 or wider, within the bound.
No kernel may reach another device: no remote copies, remote signals or barrier semaphores. Data moves between devices by JAX's collectives and lax.ppermute only.
A program may use at most 64 MiB of HBM per device.

```python
import math
import jax
import jax.numpy as jnp
import numpy as np
from jax import lax

D = 4096
FF = 7168
EXPERTS = 16
MOE_DEV = 128
MOE_TOKENS = 4096
CAP = 32
HEADS = 128
HEAD_SIZE = 64
STATE = 16
BLOCK = 256
SEQ = 16384
N_EXP = 32


def draw_step_size(key, part):
    first, second = jax.random.split(key)
    base = jax.random.uniform(first, (HEADS, SEQ), jnp.float32, math.log(0.002), math.log(0.05))
    region = jax.random.uniform(second, (HEADS, SEQ // BLOCK), jnp.float32, -1.0, 1.0)
    return jnp.exp(base + jnp.repeat(region, BLOCK, axis=1)).astype(jnp.float32)


def draw_decay_log(key, part):
    first, second, third = jax.random.split(key, 3)
    share = 0.5
    keeping = jax.random.bernoulli(first, share, (HEADS,))
    slower = jax.random.uniform(second, (HEADS,), jnp.float32, math.log(0.0001), math.log(0.0004))
    faster = jax.random.uniform(third, (HEADS,), jnp.float32, 0.0, math.log(4.0))
    return jnp.where(keeping, slower, faster).astype(jnp.float32)


def block_levels(key, shape, cuts, least, high):
    gain, own = 1.0, jax.random.fold_in(key, 6)
    for position, parts in cuts:
        draws = jnp.exp(jax.random.uniform(jax.random.fold_in(own, position), (parts,), jnp.float32, least / len(cuts), high / len(cuts)))
        gain = gain * jnp.repeat(draws, shape[position] // parts).reshape([-1 if axis == position else 1 for axis in range(len(shape))])
    return gain


def deal_out(rng, own, number, rows, count, top, bound, lean):
    ranking = jax.random.permutation(rng, count)
    crowded, ordinary = shares(count, rows * top, bound, lean, True), shares(count, rows * top, bound, lean, False)
    places = jnp.arange(count)

    def named(tallies, turn):
        used = int((tallies > 0).sum())
        fixed = max(1, used // 4)
        shifted = fixed + (places - fixed + turn * (used - fixed)) % max(1, count - fixed)
        return jnp.zeros((count,), jnp.int32).at[ranking[jnp.where(places < fixed, places, shifted)]].set(jnp.asarray(tallies, jnp.int32))

    tallies = jnp.where(number % 4 == 0, named(crowded, number // 4), named(ordinary, number - number // 4 - 1))
    mixed = jax.random.permutation(jax.random.fold_in(own, 3), count)
    source_of, sink = mixed[0:count // 2 * 2:2], mixed[1:count // 2 * 2:2]
    room = jnp.minimum(tallies[source_of] - 1, bound - tallies[sink]) // 2
    room = jnp.where((source_of == ranking[0]) | (sink == ranking[0]) | (tallies[sink] == 0), 0, jnp.maximum(room, 0))
    shifted = jax.random.randint(jax.random.fold_in(own, 4), (count // 2,), 0, 1 << 20) % (room + 1)
    tallies = tallies.at[source_of].add(-shifted).at[sink].add(shifted)
    labels = jnp.searchsorted(jnp.cumsum(tallies), jnp.arange(rows * top), side="right").astype(jnp.int32)
    table = labels.reshape(top, rows).T
    table = table[jax.random.permutation(jax.random.fold_in(own, 1), rows)]
    turn = jax.random.randint(jax.random.fold_in(own, 2), (rows, 1), 0, top)
    return jnp.take_along_axis(table, (jnp.arange(top)[None, :] + turn) % top, axis=1)


def shares(number_of, total, most, slope, full):
    weights = [(1 << 20) // math.isqrt(grade ** slope) + 1 for grade in range(1, number_of + 1)]
    largest = most if full else min(most, max(-(-total // number_of), total * weights[0] // sum(weights)))
    least = 1 if total - largest >= number_of - 1 else 0
    counts, surplus = [largest] + [least] * (number_of - 1), total - largest - least * (number_of - 1)
    while surplus > 0:
        movable = [i for i in range(1, number_of) if counts[i] < largest] or [i for i in range(1, number_of) if counts[i] < most]
        mass, remaining = sum([weights[i] for i in movable]), surplus
        for i in movable:
            extra = min(most - counts[i], max(1, remaining * weights[i] // mass), surplus)
            counts[i] = counts[i] + extra
            surplus = surplus - extra
    return np.array(counts)


def bell_draw(key, extent, width, reach, cuts=(), kind=jnp.bfloat16):
    array = jax.random.normal(key, extent, jnp.float32) * width
    if len(cuts) > 0:
        array = block_levels(key, extent, cuts, -0.22, 0.18) * array
    return jnp.clip(array, min=-reach, max=reach).astype(kind)


def setup_inputs(seed: int = 0) -> dict:
    key_list = jax.random.split(jax.random.key(seed), 13)
    seq_inputs = bell_draw(key_list[0], (SEQ, HEADS * HEAD_SIZE), 1.0, 6.0, ((0, 32), (1, 32)))
    step_size = draw_step_size(jax.random.fold_in(key_list[12], 71), 0)
    write_map = bell_draw(key_list[2], (STATE, SEQ), 0.3, 2.0, ((1, 32),))
    read_map = bell_draw(key_list[3], (STATE, SEQ), 0.3, 2.0, ((1, 32),))
    decay_log = draw_decay_log(jax.random.fold_in(key_list[12], 71), 0)
    skip_gain = jnp.clip(0.5 + 1.0 * jax.random.uniform(key_list[5], (HEADS,), jnp.float32) ** block_levels(key_list[5], (HEADS,), ((0, 32),), -0.2, 0.2), 0.5, 1.5)
    moe_tokens = bell_draw(key_list[6], (MOE_TOKENS, D), 1.0, 6.0, ((0, 32),))
    expert_ids_keys = jax.random.split(jax.random.fold_in(key_list[7], 1), MOE_TOKENS // MOE_DEV)
    expert_ids_turns = jax.random.permutation(jax.random.fold_in(key_list[7], 3), MOE_TOKENS // MOE_DEV)
    expert_ids = jax.vmap(lambda own, number: deal_out(jax.random.fold_in(key_list[7], 2), own, number, MOE_DEV, EXPERTS, 2, CAP, 2))(expert_ids_keys, expert_ids_turns).reshape((MOE_TOKENS, 2))
    route_weights = jnp.clip(0.1 + 0.9 * jax.random.uniform(key_list[8], (MOE_TOKENS, 2), jnp.float32) ** block_levels(key_list[8], (MOE_TOKENS, 2), ((0, 32),), -0.2, 0.2), 0.1, 1.0)
    gate_proj = bell_draw(key_list[9], (2 * EXPERTS, D, FF // 2), D ** -0.5, 0.09375, ((0, 32), (2, 32)))
    up_proj = bell_draw(key_list[10], (2 * EXPERTS, D, FF // 2), D ** -0.5, 0.09375, ((0, 32), (2, 32)))
    down_proj = bell_draw(key_list[11], (2 * EXPERTS, FF // 2, D), FF ** -0.5, 0.0625, ((0, 32), (2, 32)))
    return dict(seq_inputs=seq_inputs, step_size=step_size, write_map=write_map, read_map=read_map, decay_log=decay_log, skip_gain=skip_gain, moe_tokens=moe_tokens, expert_ids=expert_ids, route_weights=route_weights, gate_proj=gate_proj, up_proj=up_proj, down_proj=down_proj)


HIGHEST = lax.Precision.HIGHEST


def mixer_reference(seq_inputs, step_size, write_map, read_map, decay_log, skip_gain):
    length = seq_inputs.shape[0]
    head_count = step_size.shape[0]
    state_count = write_map.shape[0]
    head_width = seq_inputs.shape[1] // head_count
    block_count = length // BLOCK
    decay_rate = -jnp.exp(decay_log)
    log_decay = (step_size * decay_rate[:, None]).reshape(head_count, block_count, BLOCK).transpose(1, 0, 2)
    step_blocks = step_size.reshape(head_count, block_count, BLOCK).transpose(1, 0, 2)
    write_blocks = write_map.reshape(state_count, block_count, BLOCK).transpose(1, 0, 2)
    read_blocks = read_map.reshape(state_count, block_count, BLOCK).transpose(1, 0, 2)
    value_blocks = seq_inputs.reshape(block_count, BLOCK, head_count, head_width)
    row_index = lax.broadcasted_iota(jnp.int32, (BLOCK, BLOCK), 0)
    column_index = lax.broadcasted_iota(jnp.int32, (BLOCK, BLOCK), 1)
    lower = column_index <= row_index

    def one_block(running, pieces):
        log_part, step_part, write_part, read_part, value_part = pieces
        cumulative = jnp.cumsum(log_part, axis=1)
        block_end = cumulative[:, BLOCK - 1]
        scores = jnp.dot(read_part.T, write_part, preferred_element_type=jnp.float32)
        difference = cumulative[:, :, None] - cumulative[:, None, :]
        decay = jnp.where(lower[None], jnp.exp(jnp.minimum(difference, 0.0)), 0.0)
        mixing = (scores[None] * decay * step_part[:, None, :]).astype(jnp.bfloat16)
        values = value_part.astype(jnp.float32)
        local_mix = jnp.einsum("hts,shp->thp", mixing.astype(jnp.float32), values)
        carried = jnp.einsum("nt,hnp->thp", read_part.astype(jnp.float32), running, precision=HIGHEST)
        carried = carried * jnp.exp(cumulative).T[:, :, None]
        output = local_mix + carried + skip_gain[None, :, None] * values
        weights = jnp.exp(block_end[:, None] - cumulative) * step_part
        key_decayed = (write_part[None] * weights[:, None, :]).astype(jnp.bfloat16)
        increment = jnp.einsum("hns,shp->hnp", key_decayed.astype(jnp.float32), values)
        running = jnp.exp(block_end)[:, None, None] * running + increment
        return running, output.astype(jnp.bfloat16)

    zero_state = jnp.zeros((head_count, state_count, head_width), jnp.float32)
    final_state, outputs = lax.scan(one_block, zero_state, (log_decay, step_blocks, write_blocks, read_blocks, value_blocks))
    return outputs.reshape(length, head_count * head_width)


def expert_reference(moe_tokens, expert_ids, route_weights, gate_proj, up_proj, down_proj):
    total_tokens = moe_tokens.shape[0]
    model_width = moe_tokens.shape[1]
    group_size = total_tokens // N_EXP
    expert_count = gate_proj.shape[0] // 2
    assigned = expert_ids.reshape(N_EXP, group_size * 2)
    onehot = (assigned[:, :, None] == jnp.arange(expert_count, dtype=jnp.int32)[None, None, :]).astype(jnp.int32)
    earlier_count = jnp.cumsum(onehot, axis=1) - onehot
    slot_index = jnp.sum(earlier_count * onehot, axis=2).astype(jnp.int32)
    group_index = jnp.broadcast_to(jnp.arange(N_EXP, dtype=jnp.int32)[:, None], assigned.shape)
    token_index = group_index * group_size + jnp.arange(group_size * 2, dtype=jnp.int32)[None, :] // 2
    table = jnp.full((expert_count, N_EXP, CAP), total_tokens, jnp.int32)
    table = table.at[assigned, group_index, slot_index].set(token_index.astype(jnp.int32))
    padded = jnp.concatenate([moe_tokens, jnp.zeros((1, model_width), jnp.bfloat16)], axis=0)

    def run_expert(expert):
        rows_in = padded[table[expert].reshape(-1)]
        gate_full = jnp.concatenate([gate_proj[2 * expert], gate_proj[2 * expert + 1]], axis=1)
        up_full = jnp.concatenate([up_proj[2 * expert], up_proj[2 * expert + 1]], axis=1)
        down_full = jnp.concatenate([down_proj[2 * expert], down_proj[2 * expert + 1]], axis=0)
        gate_sums = jnp.dot(rows_in, gate_full, preferred_element_type=jnp.float32)
        up_sums = jnp.dot(rows_in, up_full, preferred_element_type=jnp.float32)
        hidden = (jax.nn.silu(gate_sums) * up_sums).astype(jnp.bfloat16)
        return jnp.dot(hidden, down_full, preferred_element_type=jnp.float32)

    results = lax.map(run_expert, jnp.arange(expert_count, dtype=jnp.int32))
    results = results.reshape(expert_count, N_EXP, CAP, model_width)
    picked = results[assigned, group_index, slot_index]
    weighted = picked * route_weights.reshape(N_EXP, group_size * 2)[:, :, None]
    mixed = jnp.sum(weighted.reshape(total_tokens, 2, model_width), axis=1)
    return mixed.astype(jnp.bfloat16)


def reference(seq_inputs, step_size, write_map, read_map, decay_log, skip_gain, moe_tokens, expert_ids, route_weights, gate_proj, up_proj, down_proj):
    return (mixer_reference(seq_inputs, step_size, write_map, read_map, decay_log, skip_gain),
            expert_reference(moe_tokens, expert_ids, route_weights, gate_proj, up_proj, down_proj))
```

```python
import jax
import jax.numpy as jnp
from jax import lax
from jax.sharding import PartitionSpec as P

BLOCK = 256


HIGHEST = lax.Precision.HIGHEST


def side_by_side(arrays, axis, dim, along):
    columns = [a.reshape(*a.shape[:along], -1) for a in arrays]
    both = jnp.concatenate(columns, axis=along)
    result, at, done = (lax.all_gather(both, axis, axis=dim, tiled=True), 0, [])
    for a, column in zip(arrays, columns):
        section = result[..., at : at + column.shape[along]]
        done.append(section.reshape(*section.shape[:along], *a.shape[along:]))
        at += column.shape[along]
    return tuple(done)


def block_chain(running, pieces):
    decay, increment = pieces
    return (decay[:, None, None] * running + increment, running)


def mixer_prepare(seq_inputs, step_size, write_map, read_map, decay_log):
    length = seq_inputs.shape[0]
    head_count = step_size.shape[0]
    state_count = write_map.shape[0]
    head_width = seq_inputs.shape[1] // head_count
    block_count = length // BLOCK
    decay_rate = -jnp.exp(decay_log)
    log_decay = (step_size * decay_rate[:, None]).reshape(head_count, block_count, BLOCK)
    cumulative = jnp.cumsum(log_decay, axis=2)
    block_ends = cumulative[:, :, BLOCK - 1]
    step_blocks = step_size.reshape(head_count, block_count, BLOCK)
    write_blocks = write_map.reshape(state_count, block_count, BLOCK)
    read_blocks = read_map.reshape(state_count, block_count, BLOCK)
    value_blocks = seq_inputs.reshape(block_count, BLOCK, head_count, head_width)
    scores = jnp.einsum(
        "nkt,nks->kts", read_blocks, write_blocks, preferred_element_type=jnp.float32
    )
    row_index = lax.broadcasted_iota(jnp.int32, (BLOCK, BLOCK), 0)
    column_index = lax.broadcasted_iota(jnp.int32, (BLOCK, BLOCK), 1)
    lower = column_index <= row_index
    difference = cumulative[:, :, :, None] - cumulative[:, :, None, :]
    decay = jnp.where(lower[None, None], jnp.exp(jnp.minimum(difference, 0.0)), 0.0)
    mixing = (scores[None] * decay * step_blocks[:, :, None, :]).astype(jnp.bfloat16)
    local_mix = jnp.einsum(
        "hkts,kshp->kthp", mixing, value_blocks, preferred_element_type=jnp.float32
    )
    weights = jnp.exp(block_ends[:, :, None] - cumulative) * step_blocks
    key_decayed = (write_blocks[None] * weights[:, None]).astype(jnp.bfloat16)
    increments = jnp.einsum(
        "hnks,kshp->khnp", key_decayed, value_blocks, preferred_element_type=jnp.float32
    )
    zero_state = jnp.zeros((head_count, state_count, head_width), jnp.float32)
    final, entering = lax.scan(block_chain, zero_state, (jnp.exp(block_ends).T, increments))
    return (local_mix, cumulative, block_ends, entering, final)


def mixer_finish(
    local_mix, cumulative, block_ends, entering, state_before, read_map, seq_inputs, skip_gain
):
    head_count = block_ends.shape[0]
    block_count = block_ends.shape[1]
    state_count = read_map.shape[0]
    head_width = entering.shape[3]
    before = jnp.cumsum(block_ends, axis=1) - block_ends
    states = jnp.exp(before).T[:, :, None, None] * state_before[None] + entering
    read_blocks = read_map.reshape(state_count, block_count, BLOCK).astype(jnp.float32)
    carried = jnp.einsum("nkt,khnp->kthp", read_blocks, states, precision=HIGHEST)
    carried = carried * jnp.exp(cumulative).transpose(1, 2, 0)[:, :, :, None]
    value_blocks = seq_inputs.reshape(block_count, BLOCK, head_count, head_width).astype(
        jnp.float32
    )
    output = local_mix + carried + skip_gain[None, None, :, None] * value_blocks
    return output.reshape(seq_inputs.shape).astype(jnp.bfloat16)


CTX = ("zh", "zl", "core")
SWAP = ((0, 1), (1, 0))


def swap(array, axis):
    return lax.ppermute(array, axis, SWAP)


def four(array):
    across = swap(array, "zl")
    return (array, swap(array, "core"), across, swap(across, "core"))


def absolute(pieces):
    zl = lax.axis_index("zl")
    core = lax.axis_index("core")
    first, second, third, fourth = pieces
    low = jnp.where(core == 0, first, second), jnp.where(core == 0, second, first)
    high = jnp.where(core == 0, third, fourth), jnp.where(core == 0, fourth, third)
    low = jnp.stack(low)
    high = jnp.stack(high)
    return jnp.concatenate(
        [jnp.where(zl == 0, low, high), jnp.where(zl == 0, high, low)], axis=0
    )


def route(expert_ids, route_weights, expert_count, capacity):
    group_size = expert_ids.shape[0]
    quarter = capacity // 4
    part = lax.axis_index("zl") * 2 + lax.axis_index("core")
    assigned = expert_ids.reshape(group_size * 2)
    onehot = (
        assigned[:, None] == lax.broadcasted_iota(jnp.int32, (group_size * 2, expert_count), 1)
    ).astype(jnp.int32)
    earlier_count = jnp.cumsum(onehot, axis=0) - onehot
    slot = jnp.sum(earlier_count * onehot, axis=1) - part * quarter
    position = jnp.where((slot >= 0) & (slot < quarter), assigned * quarter + slot, -1)
    matches = (
        position[:, None]
        == lax.broadcasted_iota(jnp.int32, (group_size * 2, expert_count * quarter), 1)
    ).astype(jnp.float32)
    shape = (group_size, 2, expert_count * quarter)
    dispatch = jnp.sum(matches.reshape(shape), axis=1).astype(jnp.bfloat16)
    combine = jnp.sum(
        (matches * route_weights.reshape(group_size * 2)[:, None]).reshape(shape), axis=1
    )
    return dispatch, combine


def expert_block(moe_tokens, expert_ids, route_weights, gate_proj, up_proj, down_proj):
    group_size = moe_tokens.shape[0]
    model_width = moe_tokens.shape[1]
    expert_count = lax.axis_size("exp") // 2
    capacity = min(group_size, 4 * group_size // expert_count)
    quarter = capacity // 4
    hidden_count = gate_proj.shape[2]
    dispatch, combine = route(expert_ids, route_weights, expert_count, capacity)
    weights = four(jnp.concatenate([gate_proj[0], up_proj[0]], axis=1))
    down = jnp.concatenate(four(down_proj[0]), axis=1)
    packed = jnp.einsum(
        "is,id->sd", dispatch, moe_tokens, preferred_element_type=jnp.float32
    ).astype(jnp.bfloat16)
    doubled = jnp.broadcast_to(
        packed.reshape(expert_count, 1, quarter, model_width),
        (expert_count, 2, quarter, model_width),
    )
    arrived = lax.all_to_all(
        doubled.reshape(2 * expert_count, quarter, model_width),
        "exp",
        split_axis=0,
        concat_axis=0,
        tiled=True,
    ).reshape(2 * expert_count * quarter, model_width)
    pieces = []
    for weight in weights:
        sums = lax.dot_general(
            weight, arrived, (((0,), (1,)), ((), ())), preferred_element_type=jnp.float32
        )
        pieces.append(
            (jax.nn.silu(sums[:hidden_count]) * sums[hidden_count:]).astype(jnp.bfloat16)
        )
    hidden = absolute(pieces).reshape(4 * hidden_count, -1)
    gathered = lax.all_gather(hidden, "zh", axis=0, tiled=True)
    partial_out = lax.dot_general(
        gathered, down, (((0,), (0,)), ((), ())), preferred_element_type=jnp.float32
    )
    returned = lax.all_to_all(
        partial_out.reshape(2 * expert_count, quarter, -1),
        "exp",
        split_axis=0,
        concat_axis=0,
        tiled=True,
    )
    summed = jnp.sum(returned.reshape(expert_count, 2, quarter, -1), axis=1).reshape(
        expert_count * quarter, -1
    )
    result = jnp.dot(combine, summed, precision=HIGHEST, preferred_element_type=jnp.float32)
    width = result.shape[1] // 4
    result = result.reshape(group_size, 4, width)
    received = swap(jnp.stack([result[:, 1], result[:, 3]]), "core")
    own = result[:, 0] + received[0]
    other = result[:, 2] + received[1]
    return (own + swap(other, "zl")).astype(jnp.bfloat16)


def on_device(
    seq_inputs,
    step_size,
    write_map,
    read_map,
    decay_log,
    skip_gain,
    moe_tokens,
    expert_ids,
    route_weights,
    gate_proj,
    up_proj,
    down_proj,
):
    local_mix, cumulative, block_ends, entering, final = mixer_prepare(
        seq_inputs, step_size, write_map, read_map, decay_log
    )
    total_log = jnp.sum(block_ends, axis=1)
    group_count = lax.axis_size(CTX)
    all_logs, all_states = side_by_side((total_log[None], final[None]), CTX, 0, 2)
    position_here = lax.axis_index(CTX)
    source = lax.broadcasted_iota(jnp.int32, (group_count, group_count), 0)
    target = lax.broadcasted_iota(jnp.int32, (group_count, group_count), 1)
    between = ((target > source) & (target < position_here)).astype(jnp.float32)
    log_span = jnp.dot(between, all_logs, precision=HIGHEST, preferred_element_type=jnp.float32)
    earlier = lax.broadcasted_iota(jnp.int32, (group_count, 1), 0) < position_here
    factor = jnp.where(earlier, jnp.exp(log_span), 0.0)
    state_before = jnp.einsum("jh,jhnp->hnp", factor, all_states, precision=HIGHEST)
    expert_output = expert_block(
        moe_tokens, expert_ids, route_weights, gate_proj, up_proj, down_proj
    )
    mixer_output = mixer_finish(
        local_mix, cumulative, block_ends, entering, state_before, read_map, seq_inputs, skip_gain
    )
    return (mixer_output, expert_output)


def solution(mesh):
    devices = mesh.devices
    ctx_size, exp_size = devices.shape
    split = jax.sharding.Mesh(
        devices.reshape(ctx_size // 4, 2, 2, exp_size), ("zh", "zl", "core", "exp")
    )
    return jax.shard_map(
        on_device,
        mesh=split,
        in_specs=(
            P(CTX, "exp"),
            P("exp", CTX),
            P(None, CTX),
            P(None, CTX),
            P("exp"),
            P("exp"),
            P("exp", None),
            P("exp", None),
            P("exp", None),
            P("exp", None, CTX),
            P("exp", None, CTX),
            P("exp", None, CTX),
        ),
        out_specs=(P(CTX, "exp"), P("exp", CTX)),
        check_vma=False,
    )
```

```python
import jax
import jax.numpy as jnp
from jax import lax
from jax.sharding import PartitionSpec as P

BLOCK = 256


HIGHEST = lax.Precision.HIGHEST


def side_by_side(arrays, axis, dim, along):
    columns = [a.reshape(*a.shape[:along], -1) for a in arrays]
    both = jnp.concatenate(columns, axis=along)
    result, at, done = (lax.all_gather(both, axis, axis=dim, tiled=True), 0, [])
    for a, column in zip(arrays, columns):
        section = result[..., at : at + column.shape[along]]
        done.append(section.reshape(*section.shape[:along], *a.shape[along:]))
        at += column.shape[along]
    return tuple(done)


def block_chain(running, pieces):
    decay, increment = pieces
    return (decay[:, None, None] * running + increment, running)


def mixer_prepare(seq_inputs, step_size, write_map, read_map, decay_log):
    length = seq_inputs.shape[0]
    head_count = step_size.shape[0]
    state_count = write_map.shape[0]
    head_width = seq_inputs.shape[1] // head_count
    block_count = length // BLOCK
    decay_rate = -jnp.exp(decay_log)
    log_decay = (step_size * decay_rate[:, None]).reshape(head_count, block_count, BLOCK)
    cumulative = jnp.cumsum(log_decay, axis=2)
    block_ends = cumulative[:, :, BLOCK - 1]
    step_blocks = step_size.reshape(head_count, block_count, BLOCK)
    write_blocks = write_map.reshape(state_count, block_count, BLOCK)
    read_blocks = read_map.reshape(state_count, block_count, BLOCK)
    value_blocks = seq_inputs.reshape(block_count, BLOCK, head_count, head_width)
    scores = jnp.einsum(
        "nkt,nks->kts", read_blocks, write_blocks, preferred_element_type=jnp.float32
    )
    row_index = lax.broadcasted_iota(jnp.int32, (BLOCK, BLOCK), 0)
    column_index = lax.broadcasted_iota(jnp.int32, (BLOCK, BLOCK), 1)
    lower = column_index <= row_index
    difference = cumulative[:, :, :, None] - cumulative[:, :, None, :]
    decay = jnp.where(lower[None, None], jnp.exp(jnp.minimum(difference, 0.0)), 0.0)
    mixing = (scores[None] * decay * step_blocks[:, :, None, :]).astype(jnp.bfloat16)
    local_mix = jnp.einsum(
        "hkts,kshp->kthp", mixing, value_blocks, preferred_element_type=jnp.float32
    )
    weights = jnp.exp(block_ends[:, :, None] - cumulative) * step_blocks
    key_decayed = (write_blocks[None] * weights[:, None]).astype(jnp.bfloat16)
    increments = jnp.einsum(
        "hnks,kshp->khnp", key_decayed, value_blocks, preferred_element_type=jnp.float32
    )
    zero_state = jnp.zeros((head_count, state_count, head_width), jnp.float32)
    final, entering = lax.scan(block_chain, zero_state, (jnp.exp(block_ends).T, increments))
    return (local_mix, cumulative, block_ends, entering, final)


def mixer_finish(
    local_mix, cumulative, block_ends, entering, state_before, read_map, seq_inputs, skip_gain
):
    head_count = block_ends.shape[0]
    block_count = block_ends.shape[1]
    state_count = read_map.shape[0]
    head_width = entering.shape[3]
    before = jnp.cumsum(block_ends, axis=1) - block_ends
    states = jnp.exp(before).T[:, :, None, None] * state_before[None] + entering
    read_blocks = read_map.reshape(state_count, block_count, BLOCK).astype(jnp.float32)
    carried = jnp.einsum("nkt,khnp->kthp", read_blocks, states, precision=HIGHEST)
    carried = carried * jnp.exp(cumulative).transpose(1, 2, 0)[:, :, :, None]
    value_blocks = seq_inputs.reshape(block_count, BLOCK, head_count, head_width).astype(
        jnp.float32
    )
    output = local_mix + carried + skip_gain[None, None, :, None] * value_blocks
    return output.reshape(seq_inputs.shape).astype(jnp.bfloat16)


CTX = ("zh", "zl", "core")
SWAP = ((0, 1), (1, 0))
CHUNKS = 1


def swap(array, axis):
    return lax.ppermute(array, axis, SWAP)


def four(array, across):
    beside = swap(array, "core")
    return (array, beside, across, swap(across, "core"))


def ring(array):
    count = lax.axis_size("zh")
    rows = array.shape[0]
    ahead = [(i, (i + 1) % count) for i in range(count)]
    behind = [(i, (i - 1) % count) for i in range(count)]
    yield 0, 0, array
    forward, backward = array, array
    for step in range(1, count // 2):
        forward = lax.ppermute(forward, "zh", ahead)
        backward = lax.ppermute(backward, "zh", behind)
        yield -step, 0, forward
        yield step, 0, backward
    half = rows // 2
    yield -(count // 2), 0, lax.ppermute(forward[:half], "zh", ahead)
    yield count // 2, half, lax.ppermute(backward[half:], "zh", behind)


def absolute(pieces):
    zl = lax.axis_index("zl")
    core = lax.axis_index("core")
    first, second, third, fourth = pieces
    low = jnp.where(core == 0, first, second), jnp.where(core == 0, second, first)
    high = jnp.where(core == 0, third, fourth), jnp.where(core == 0, fourth, third)
    low = jnp.stack(low)
    high = jnp.stack(high)
    return jnp.concatenate(
        [jnp.where(zl == 0, low, high), jnp.where(zl == 0, high, low)], axis=0
    )


def joined(first, second):
    return first[0] + second[0], jnp.exp(second[0])[:, None, None] * first[1] + second[1]


def exchanged(pair, axis):
    log, state = pair
    both = jnp.concatenate([log[:, None], state.reshape(state.shape[0], -1)], axis=1)
    received = swap(both, axis)
    return received[:, 0], received[:, 1:].reshape(state.shape)


def chosen(flag, left, right):
    return jax.tree.map(lambda a, b: jnp.where(flag, a, b), left, right)


def carry(total_log, final):
    own = (total_log, final)
    before = jax.tree.map(jnp.zeros_like, own)
    for axis in ("core", "zl"):
        other = exchanged(own, axis)
        later = lax.axis_index(axis) == 1
        before = chosen(later, joined(other, before), before)
        own = chosen(later, joined(other, own), joined(own, other))
    logs, states = side_by_side((own[0][None], own[1][None]), "zh", 0, 2)
    count = lax.axis_size("zh")
    place = lax.axis_index("zh")
    source = lax.broadcasted_iota(jnp.int32, (count, count), 0)
    target = lax.broadcasted_iota(jnp.int32, (count, count), 1)
    between = ((target > source) & (target < place)).astype(jnp.float32)
    log_span = jnp.dot(between, logs, precision=HIGHEST, preferred_element_type=jnp.float32)
    earlier = lax.broadcasted_iota(jnp.int32, (count, 1), 0) < place
    factor = jnp.where(earlier, jnp.exp(log_span), 0.0)
    outside = jnp.sum(factor[:, :, None, None] * states, axis=0)
    return joined((jnp.zeros_like(total_log), outside), before)[1]


def route(expert_ids, route_weights, expert_count, rows):
    group_size = expert_ids.shape[0]
    quarter = CHUNKS * rows
    part = lax.axis_index("zl") * 2 + lax.axis_index("core")
    assigned = expert_ids.reshape(group_size * 2)
    onehot = (
        assigned[:, None] == lax.broadcasted_iota(jnp.int32, (group_size * 2, expert_count), 1)
    ).astype(jnp.int32)
    earlier_count = jnp.cumsum(onehot, axis=0) - onehot
    slot = jnp.sum(earlier_count * onehot, axis=1) - part * quarter
    position = jnp.where((slot >= 0) & (slot < quarter), assigned * quarter + slot, -1)
    matches = (
        position[:, None]
        == lax.broadcasted_iota(jnp.int32, (group_size * 2, expert_count * quarter), 1)
    ).astype(jnp.float32)
    shape = (group_size, 2, expert_count, CHUNKS, rows)
    dispatch = jnp.sum(matches.reshape(shape), axis=1).astype(jnp.bfloat16)
    combine = jnp.sum(
        (matches * route_weights.reshape(group_size * 2)[:, None]).reshape(shape), axis=1
    )
    return dispatch, combine


def exchange(array):
    return lax.all_to_all(array, "exp", split_axis=0, concat_axis=0, tiled=True)


def send_slots(moe_tokens, dispatch):
    group_size, expert_count, _, rows = dispatch.shape
    packed = []
    for chunk in range(CHUNKS):
        onehot = jnp.broadcast_to(
            dispatch[:, :, chunk, :][:, :, None, :], (group_size, expert_count, 2, rows)
        )
        packed.append(
            jnp.einsum(
                "iehs,id->ehsd", onehot, moe_tokens, preferred_element_type=jnp.float32
            )
            .astype(jnp.bfloat16)
            .reshape(2 * expert_count, rows, -1)
        )
    return packed


def hidden_units(arrived, weights, hidden_count):
    pieces = []
    for weight in weights:
        sums = lax.dot_general(
            weight, arrived, (((0,), (1,)), ((), ())), preferred_element_type=jnp.float32
        ).reshape(2, 2, hidden_count, -1)
        acted = (jax.nn.silu(sums[:, 0]) * sums[:, 1]).astype(jnp.bfloat16)
        pieces.extend((acted[0], acted[1]))
    return absolute(pieces).reshape(4 * hidden_count, -1)


def down_sums(hidden, down):
    place = lax.axis_index("zh")
    count = lax.axis_size("zh")
    size = hidden.shape[0]
    total = 0.0
    for offset, first, shard in ring(hidden):
        start = (place + (offset + count)) % count * size + first
        rows = lax.dynamic_slice_in_dim(down, start, shard.shape[0], 0)
        total = total + lax.dot_general(
            shard, rows, (((0,), (0,)), ((), ())), preferred_element_type=jnp.float32
        )
    return total


def combined(returned, combine):
    group_size, expert_count, rows = combine.shape
    summed = jnp.sum(returned.reshape(expert_count, 2, rows, -1), axis=1)
    return jnp.dot(
        combine.reshape(group_size, expert_count * rows),
        summed.reshape(expert_count * rows, -1),
        precision=HIGHEST,
        preferred_element_type=jnp.float32,
    )


def shared_out(result):
    width = result.shape[1] // 4
    total = result[:, :width]
    for r in (3, 2, 1):
        total = total + lax.ppermute(
            result[:, r * width : (r + 1) * width], ("zl", "core"), [(i, i ^ r) for i in range(4)]
        )
    return total.astype(jnp.bfloat16)


def layer(
    seq_inputs,
    step_size,
    write_map,
    read_map,
    decay_log,
    skip_gain,
    moe_tokens,
    expert_ids,
    route_weights,
    gate_proj,
    up_proj,
    down_proj,
):
    expert_count = lax.axis_size("exp") // 2
    rows = min(moe_tokens.shape[0], 4 * moe_tokens.shape[0] // expert_count) // 4 // CHUNKS
    hidden_count = gate_proj.shape[2]
    gate, up, down = gate_proj[0], up_proj[0], down_proj[0]
    gate_across = swap(gate, "zl")
    up_across = swap(up, "zl")
    dispatch, combine = route(expert_ids, route_weights, expert_count, rows)
    packed = send_slots(moe_tokens, dispatch)
    packed, gate, up, down, seq_inputs, step_size = lax.optimization_barrier(
        (packed, gate, up, down, seq_inputs, step_size)
    )
    arrived = [exchange(chunk) for chunk in packed]
    down_across = swap(down, "zl")
    gates = four(gate, gate_across)
    ups = four(up, up_across)
    weights = [
        jnp.concatenate([gates[r], ups[r], gates[r + 1], ups[r + 1]], axis=1) for r in (0, 2)
    ]
    down_columns = jnp.concatenate(four(down, down_across), axis=1)
    local_mix, cumulative, block_ends, entering, final = mixer_prepare(
        seq_inputs, step_size, write_map, read_map, decay_log
    )
    sums = [
        down_sums(
            hidden_units(a.reshape(2 * expert_count * rows, -1), weights, hidden_count),
            down_columns,
        )
        for a in arrived
    ]
    total_log = jnp.sum(block_ends, axis=1)
    returned = [exchange(part.reshape(2 * expert_count, rows, -1)) for part in sums]
    state_before = carry(total_log, final)
    mixer_output = mixer_finish(
        local_mix, cumulative, block_ends, entering, state_before, read_map, seq_inputs, skip_gain
    )
    result = sum(combined(part, combine[:, :, chunk]) for chunk, part in enumerate(returned))
    expert_output = shared_out(result)
    return (mixer_output, expert_output)


def solution(mesh):
    devices = mesh.devices
    ctx_size, exp_size = devices.shape
    split = jax.sharding.Mesh(
        devices.reshape(ctx_size // 4, 2, 2, exp_size), ("zh", "zl", "core", "exp")
    )
    return jax.shard_map(
        layer,
        mesh=split,
        in_specs=(
            P(CTX, "exp"),
            P("exp", CTX),
            P(None, CTX),
            P(None, CTX),
            P("exp"),
            P("exp"),
            P("exp", None),
            P("exp", None),
            P("exp", None),
            P("exp", None, CTX),
            P("exp", None, CTX),
            P("exp", None, CTX),
        ),
        out_specs=(P(CTX, "exp"), P("exp", CTX)),
        check_vma=False,
    )
```

```python
import jax
import jax.numpy as jnp
from jax import lax
from jax.sharding import PartitionSpec as P

BLOCK = 256


HIGHEST = lax.Precision.HIGHEST


def block_chain(running, pieces):
    decay, increment = pieces
    return (decay[:, None, None] * running + increment, running)


def mixer_prepare(seq_inputs, step_size, write_map, read_map, decay_log):
    length = seq_inputs.shape[0]
    head_count = step_size.shape[0]
    state_count = write_map.shape[0]
    head_width = seq_inputs.shape[1] // head_count
    block_count = length // BLOCK
    decay_rate = -jnp.exp(decay_log)
    log_decay = (step_size * decay_rate[:, None]).reshape(head_count, block_count, BLOCK)
    cumulative = jnp.cumsum(log_decay, axis=2)
    block_ends = cumulative[:, :, BLOCK - 1]
    step_blocks = step_size.reshape(head_count, block_count, BLOCK)
    write_blocks = write_map.reshape(state_count, block_count, BLOCK)
    read_blocks = read_map.reshape(state_count, block_count, BLOCK)
    value_blocks = seq_inputs.reshape(block_count, BLOCK, head_count, head_width)
    scores = jnp.einsum(
        "nkt,nks->kts", read_blocks, write_blocks, preferred_element_type=jnp.float32
    )
    row_index = lax.broadcasted_iota(jnp.int32, (BLOCK, BLOCK), 0)
    column_index = lax.broadcasted_iota(jnp.int32, (BLOCK, BLOCK), 1)
    lower = column_index <= row_index
    difference = cumulative[:, :, :, None] - cumulative[:, :, None, :]
    decay = jnp.where(lower[None, None], jnp.exp(jnp.minimum(difference, 0.0)), 0.0)
    mixing = (scores[None] * decay * step_blocks[:, :, None, :]).astype(jnp.bfloat16)
    local_mix = jnp.einsum(
        "hkts,kshp->kthp", mixing, value_blocks, preferred_element_type=jnp.float32
    )
    weights = jnp.exp(block_ends[:, :, None] - cumulative) * step_blocks
    key_decayed = (write_blocks[None] * weights[:, None]).astype(jnp.bfloat16)
    increments = jnp.einsum(
        "hnks,kshp->khnp", key_decayed, value_blocks, preferred_element_type=jnp.float32
    )
    zero_state = jnp.zeros((head_count, state_count, head_width), jnp.float32)
    final, entering = lax.scan(block_chain, zero_state, (jnp.exp(block_ends).T, increments))
    return (local_mix, cumulative, block_ends, entering, final)


def mixer_finish(
    local_mix, cumulative, block_ends, entering, state_before, read_map, seq_inputs, skip_gain
):
    head_count = block_ends.shape[0]
    block_count = block_ends.shape[1]
    state_count = read_map.shape[0]
    head_width = entering.shape[3]
    before = jnp.cumsum(block_ends, axis=1) - block_ends
    states = jnp.exp(before).T[:, :, None, None] * state_before[None] + entering
    read_blocks = read_map.reshape(state_count, block_count, BLOCK).astype(jnp.float32)
    carried = jnp.einsum("nkt,khnp->kthp", read_blocks, states, precision=HIGHEST)
    carried = carried * jnp.exp(cumulative).transpose(1, 2, 0)[:, :, :, None]
    value_blocks = seq_inputs.reshape(block_count, BLOCK, head_count, head_width).astype(
        jnp.float32
    )
    output = local_mix + carried + skip_gain[None, None, :, None] * value_blocks
    return output.reshape(seq_inputs.shape).astype(jnp.bfloat16)


CTX = ("zh", "zl", "core")
SWAP = ((0, 1), (1, 0))


def swap(array, axis):
    return lax.ppermute(array, axis, SWAP)


def four(array, across):
    beside = swap(array, "core")
    return (array, beside, across, swap(across, "core"))


def absolute(pieces):
    zl = lax.axis_index("zl")
    core = lax.axis_index("core")
    first, second, third, fourth = pieces
    low = jnp.where(core == 0, first, second), jnp.where(core == 0, second, first)
    high = jnp.where(core == 0, third, fourth), jnp.where(core == 0, fourth, third)
    low = jnp.stack(low)
    high = jnp.stack(high)
    return jnp.concatenate(
        [jnp.where(zl == 0, low, high), jnp.where(zl == 0, high, low)], axis=0
    )


def joined(first, second):
    return first[0] + second[0], jnp.exp(second[0])[:, None, None] * first[1] + second[1]


def exchanged(pair, axis):
    log, state = pair
    both = jnp.concatenate([log[:, None], state.reshape(state.shape[0], -1)], axis=1)
    received = swap(both, axis)
    return received[:, 0], received[:, 1:].reshape(state.shape)


def chosen(flag, left, right):
    return jax.tree.map(lambda a, b: jnp.where(flag, a, b), left, right)


def group_state(total_log, final):
    own = (total_log, final)
    before = jax.tree.map(jnp.zeros_like, own)
    for axis in ("core", "zl"):
        other = exchanged(own, axis)
        later = lax.axis_index(axis) == 1
        before = chosen(later, joined(other, before), before)
        own = chosen(later, joined(other, own), joined(own, other))
    return own, before


def upper(array):
    return lax.reduce_precision(array, 8, 7)


def state_rows(log, state, width):
    flat = state.reshape(-1, width)
    high = upper(flat)
    first = upper(log)
    second = upper(log - first)
    logs = jnp.stack([first, second, log - first - second])
    logs = jnp.pad(logs, ((0, flat.shape[0] - 3), (0, width - log.shape[0])))
    return jnp.concatenate([high, flat - high, logs], axis=0).astype(jnp.bfloat16)


def read_rows(rows, shape):
    count, _, width = rows.shape
    parts = rows.reshape(count, 3, -1, width).astype(jnp.float32)
    logs = jnp.sum(parts[:, 2, :3, : shape[0]], axis=1)
    return logs, (parts[:, 0] + parts[:, 1]).reshape(count, *shape)


def state_ahead(offsets, logs, states, before):
    place = lax.axis_index("zh")
    count = lax.axis_size("zh")
    source = (place + jnp.array([o + count for o in offsets], jnp.int32)) % count
    earlier = source < place
    between = (source[None, :] > source[:, None]) & earlier[None, :]
    span = jnp.sum(jnp.where(between[:, :, None], logs[None], 0.0), axis=1)
    factor = jnp.where(earlier[:, None], jnp.exp(span), 0.0)
    outside = jnp.sum(factor[:, :, None, None] * states, axis=0)
    return joined((jnp.zeros_like(before[0]), outside), before)[1]


def route(expert_ids, route_weights, expert_count, capacity):
    group_size = expert_ids.shape[0]
    quarter = capacity // 4
    part = lax.axis_index("zl") * 2 + lax.axis_index("core")
    assigned = expert_ids.reshape(group_size * 2)
    onehot = (
        assigned[:, None] == lax.broadcasted_iota(jnp.int32, (group_size * 2, expert_count), 1)
    ).astype(jnp.int32)
    earlier_count = jnp.cumsum(onehot, axis=0) - onehot
    slot = jnp.sum(earlier_count * onehot, axis=1)
    ours = slot - part * quarter
    place = jnp.where((ours >= 0) & (ours < quarter), assigned * quarter + ours, -1)

    def matches(position, count):
        return (
            position[:, None] == lax.broadcasted_iota(jnp.int32, (group_size * 2, count), 1)
        ).astype(jnp.float32)

    dispatch = jnp.sum(
        matches(place, expert_count * quarter).reshape(group_size, 2, -1), axis=1
    ).astype(jnp.bfloat16)
    combine = jnp.sum(
        (
            matches(assigned * capacity + slot, expert_count * capacity)
            * route_weights.reshape(group_size * 2)[:, None]
        ).reshape(group_size, 2, -1),
        axis=1,
    )
    return dispatch.reshape(group_size, expert_count, quarter), combine


def packed_slots(moe_tokens, dispatch):
    group_size, expert_count, rows = dispatch.shape
    onehot = jnp.broadcast_to(dispatch[:, :, None, :], (group_size, expert_count, 2, rows))
    packed = jnp.einsum("iehs,id->ehsd", onehot, moe_tokens, preferred_element_type=jnp.float32)
    return packed.astype(jnp.bfloat16).reshape(2 * expert_count, rows, -1)


def hidden_units(arrived, weights, hidden_count):
    pieces = []
    for weight in weights:
        sums = lax.dot_general(
            weight, arrived, (((0,), (1,)), ((), ())), preferred_element_type=jnp.float32
        ).reshape(2, 2, hidden_count, -1)
        acted = (jax.nn.silu(sums[:, 0]) * sums[:, 1]).astype(jnp.bfloat16)
        pieces.extend((acted[0], acted[1]))
    return absolute(pieces).reshape(4 * hidden_count, -1)


def down_sums(hidden, extra, down):
    place = lax.axis_index("zh")
    count = lax.axis_size("zh")
    size = hidden.shape[0]
    head = extra.shape[0]
    ahead = [(i, (i + 1) % count) for i in range(count)]
    behind = [(i, (i - 1) % count) for i in range(count)]

    def product(offset, first, shard):
        start = (place + (offset + count)) % count * size + first
        rows = lax.dynamic_slice_in_dim(down, start, shard.shape[0], 0)
        return lax.dot_general(
            shard, rows, (((0,), (0,)), ((), ())), preferred_element_type=jnp.float32
        )

    def both(step, near):
        return product(-step, 0, near[0][head:]) + product(step, 0, near[1][head:])

    forward = backward = jnp.concatenate([extra, hidden], axis=0)
    offsets, extras = [], []
    total = product(0, 0, hidden)
    last = count // 2
    for step in range(1, last):
        forward = lax.ppermute(forward, "zh", ahead)
        backward = lax.ppermute(backward, "zh", behind)
        offsets += [-step, step]
        extras += [forward, backward]
        total = total + both(step, (forward, backward))
    half = (size + head) // 32 * 16
    forward = lax.ppermute(forward[:half], "zh", ahead)
    backward = lax.ppermute(backward[half:], "zh", behind)
    offsets.append(-last)
    extras.append(forward)
    total = total + product(-last, 0, forward[head:]) + product(last, half - head, backward)
    return total, offsets, extras


def ordered(blocks):
    for axis, dim in (("zl", 0), ("core", 1)):
        blocks = jnp.where(lax.axis_index(axis) == 0, blocks, jnp.flip(blocks, dim))
    return blocks


def layer(
    seq_inputs,
    step_size,
    write_map,
    read_map,
    decay_log,
    skip_gain,
    moe_tokens,
    expert_ids,
    route_weights,
    gate_proj,
    up_proj,
    down_proj,
):
    group_size = moe_tokens.shape[0]
    expert_count = lax.axis_size("exp") // 2
    capacity = min(group_size, 4 * group_size // expert_count)
    rows = capacity // 4
    hidden_count = gate_proj.shape[2]
    gate, up, down = gate_proj[0], up_proj[0], down_proj[0]
    gate_across = swap(gate, "zl")
    dispatch, combine = route(expert_ids, route_weights, expert_count, capacity)
    packed = packed_slots(moe_tokens, dispatch)
    packed, gate, up, down, seq_inputs, step_size = lax.optimization_barrier(
        (packed, gate, up, down, seq_inputs, step_size)
    )
    arrived = lax.all_to_all(packed, "exp", split_axis=0, concat_axis=0, tiled=True)
    up_across = swap(up, "zl")
    down_across = swap(down, "zl")
    gates = four(gate, gate_across)
    ups = four(up, up_across)
    weights = [
        jnp.concatenate([gates[r], ups[r], gates[r + 1], ups[r + 1]], axis=1) for r in (0, 2)
    ]
    down_columns = jnp.concatenate(four(down, down_across), axis=1)
    local_mix, cumulative, block_ends, entering, final = mixer_prepare(
        seq_inputs, step_size, write_map, read_map, decay_log
    )
    group, before = group_state(jnp.sum(block_ends, axis=1), final)
    hidden = hidden_units(arrived.reshape(2 * expert_count * rows, -1), weights, hidden_count)
    state_part = state_rows(*group, hidden.shape[1])
    sums, offsets, extras = down_sums(hidden, state_part, down_columns)
    width = down.shape[1]
    blocks = sums.reshape(2 * expert_count, rows, 4, width).transpose(2, 0, 1, 3)
    blocks = ordered(blocks.reshape(2, 2, 2 * expert_count, rows, width))
    blocks = blocks.transpose(2, 0, 1, 3, 4).reshape(8 * expert_count, rows, width)
    blocks, *extras = lax.optimization_barrier((blocks, *extras))
    returned = lax.all_to_all(
        blocks, ("exp", "zl", "core"), split_axis=0, concat_axis=0, tiled=True
    )
    head = state_part.shape[0]
    states = jnp.stack([message[:head] for message in extras])
    state_before = state_ahead(offsets, *read_rows(states, final.shape), before)
    mixer_output = mixer_finish(
        local_mix, cumulative, block_ends, entering, state_before, read_map, seq_inputs, skip_gain
    )
    summed = jnp.sum(returned.reshape(expert_count, 2, capacity, width), axis=1)
    expert_output = jnp.dot(
        combine,
        summed.reshape(expert_count * capacity, width),
        precision=HIGHEST,
        preferred_element_type=jnp.float32,
    ).astype(jnp.bfloat16)
    return (mixer_output, expert_output)


def solution(mesh):
    devices = mesh.devices
    ctx_size, exp_size = devices.shape
    split = jax.sharding.Mesh(
        devices.reshape(ctx_size // 4, 2, 2, exp_size), ("zh", "zl", "core", "exp")
    )
    return jax.shard_map(
        layer,
        mesh=split,
        in_specs=(
            P(CTX, "exp"),
            P("exp", CTX),
            P(None, CTX),
            P(None, CTX),
            P("exp"),
            P("exp"),
            P("exp", None),
            P("exp", None),
            P("exp", None),
            P("exp", None, CTX),
            P("exp", None, CTX),
            P("exp", None, CTX),
        ),
        out_specs=(P(CTX, "exp"), P("exp", CTX)),
        check_vma=False,
    )
```

```python
import jax
import jax.numpy as jnp
from jax import lax
from jax.experimental import pallas as pl
from jax.experimental.pallas import tpu as pltpu
from jax.sharding import PartitionSpec as P

BLOCK = 256


HIGHEST = lax.Precision.HIGHEST


def block_chain(running, pieces):
    decay, increment = pieces
    return (decay[:, None, None] * running + increment, running)


def mixer_prepare(seq_inputs, step_size, write_map, read_map, decay_log):
    length = seq_inputs.shape[0]
    head_count = step_size.shape[0]
    state_count = write_map.shape[0]
    head_width = seq_inputs.shape[1] // head_count
    block_count = length // BLOCK
    decay_rate = -jnp.exp(decay_log)
    log_decay = (step_size * decay_rate[:, None]).reshape(head_count, block_count, BLOCK)
    cumulative = jnp.cumsum(log_decay, axis=2)
    block_ends = cumulative[:, :, BLOCK - 1]
    step_blocks = step_size.reshape(head_count, block_count, BLOCK)
    write_blocks = write_map.reshape(state_count, block_count, BLOCK)
    read_blocks = read_map.reshape(state_count, block_count, BLOCK)
    value_blocks = seq_inputs.reshape(block_count, BLOCK, head_count, head_width)
    scores = jnp.einsum(
        "nkt,nks->kts", read_blocks, write_blocks, preferred_element_type=jnp.float32
    )
    row_index = lax.broadcasted_iota(jnp.int32, (BLOCK, BLOCK), 0)
    column_index = lax.broadcasted_iota(jnp.int32, (BLOCK, BLOCK), 1)
    lower = column_index <= row_index
    difference = cumulative[:, :, :, None] - cumulative[:, :, None, :]
    decay = jnp.where(lower[None, None], jnp.exp(jnp.minimum(difference, 0.0)), 0.0)
    mixing = (scores[None] * decay * step_blocks[:, :, None, :]).astype(jnp.bfloat16)
    local_mix = jnp.einsum(
        "hkts,kshp->kthp", mixing, value_blocks, preferred_element_type=jnp.float32
    )
    weights = jnp.exp(block_ends[:, :, None] - cumulative) * step_blocks
    key_decayed = (write_blocks[None] * weights[:, None]).astype(jnp.bfloat16)
    increments = jnp.einsum(
        "hnks,kshp->khnp", key_decayed, value_blocks, preferred_element_type=jnp.float32
    )
    zero_state = jnp.zeros((head_count, state_count, head_width), jnp.float32)
    final, entering = lax.scan(block_chain, zero_state, (jnp.exp(block_ends).T, increments))
    return (local_mix, cumulative, block_ends, entering, final)


def mixer_finish(
    local_mix, cumulative, block_ends, entering, state_before, read_map, seq_inputs, skip_gain
):
    head_count = block_ends.shape[0]
    block_count = block_ends.shape[1]
    state_count = read_map.shape[0]
    head_width = entering.shape[3]
    before = jnp.cumsum(block_ends, axis=1) - block_ends
    states = jnp.exp(before).T[:, :, None, None] * state_before[None] + entering
    read_blocks = read_map.reshape(state_count, block_count, BLOCK).astype(jnp.float32)
    carried = jnp.einsum("nkt,khnp->kthp", read_blocks, states, precision=HIGHEST)
    carried = carried * jnp.exp(cumulative).transpose(1, 2, 0)[:, :, :, None]
    value_blocks = seq_inputs.reshape(block_count, BLOCK, head_count, head_width).astype(
        jnp.float32
    )
    output = local_mix + carried + skip_gain[None, None, :, None] * value_blocks
    return output.reshape(seq_inputs.shape).astype(jnp.bfloat16)


CTX = ("zh", "zl", "core")
SWAP = ((0, 1), (1, 0))
SLOTS = 8


def swap(array, axis):
    return lax.ppermute(array, axis, SWAP)


def four(array, across):
    beside = swap(array, "core")
    return (array, beside, across, swap(across, "core"))


def joined(first, second):
    return first[0] + second[0], jnp.exp(second[0])[:, None, None] * first[1] + second[1]


def exchanged(pair, axis):
    log, state = pair
    both = jnp.concatenate([log[:, None], state.reshape(state.shape[0], -1)], axis=1)
    received = swap(both, axis)
    return received[:, 0], received[:, 1:].reshape(state.shape)


def chosen(flag, left, right):
    return jax.tree.map(lambda a, b: jnp.where(flag, a, b), left, right)


def group_state(total_log, final):
    own = (total_log, final)
    before = jax.tree.map(jnp.zeros_like, own)
    for axis in ("core", "zl"):
        other = exchanged(own, axis)
        later = lax.axis_index(axis) == 1
        before = chosen(later, joined(other, before), before)
        own = chosen(later, joined(other, own), joined(own, other))
    return own, before


def upper(array):
    return lax.reduce_precision(array, 8, 7)


def state_rows(log, state, width):
    flat = state.reshape(-1, width)
    high = upper(flat)
    first = upper(log)
    second = upper(log - first)
    logs = jnp.stack([first, second, log - first - second])
    logs = jnp.pad(logs, ((0, flat.shape[0] - 3), (0, width - log.shape[0])))
    return jnp.concatenate([high, flat - high, logs], axis=0).astype(jnp.bfloat16)


def read_rows(rows, shape):
    count, _, width = rows.shape
    parts = rows.reshape(count, 3, -1, width).astype(jnp.float32)
    logs = jnp.sum(parts[:, 2, :3, : shape[0]], axis=1)
    return logs, (parts[:, 0] + parts[:, 1]).reshape(count, *shape)


def state_ahead(offsets, logs, states, before):
    place = lax.axis_index("zh")
    count = lax.axis_size("zh")
    source = (place + jnp.array([o + count for o in offsets], jnp.int32)) % count
    earlier = source < place
    between = (source[None, :] > source[:, None]) & earlier[None, :]
    span = jnp.sum(jnp.where(between[:, :, None], logs[None], 0.0), axis=1)
    factor = jnp.where(earlier[:, None], jnp.exp(span), 0.0)
    outside = jnp.sum(factor[:, :, None, None] * states, axis=0)
    return joined((jnp.zeros_like(before[0]), outside), before)[1]


def combine_map(expert_ids, route_weights, expert_count, capacity):
    group_size = expert_ids.shape[0]
    assigned = expert_ids.reshape(group_size * 2)
    onehot = (
        assigned[:, None] == lax.broadcasted_iota(jnp.int32, (group_size * 2, expert_count), 1)
    ).astype(jnp.int32)
    earlier_count = jnp.cumsum(onehot, axis=0) - onehot
    position = jnp.sum((earlier_count + assigned[:, None] * capacity) * onehot, axis=1)
    matches = (
        position[:, None]
        == lax.broadcasted_iota(jnp.int32, (group_size * 2, expert_count * capacity), 1)
    ).astype(jnp.float32)
    return jnp.sum(
        (matches * route_weights.reshape(group_size * 2)[:, None]).reshape(group_size, 2, -1),
        axis=1,
    )


def pack_kernel(part_ref, ids_ref, tokens_ref, out_ref, onehot_ref):
    group_size = tokens_ref.shape[0]
    row_count = out_ref.shape[0]
    expert_count = row_count // (2 * SLOTS)

    @pl.when(pl.program_id(0) == 0)
    def _():
        shape = (expert_count, group_size)
        expert = lax.broadcasted_iota(jnp.int32, shape, 0)
        named = (ids_ref[0:1, :] == expert) | (ids_ref[1:2, :] == expert)
        named = jnp.where(named, 1.0, 0.0)
        square = (group_size, group_size)
        earlier = lax.broadcasted_iota(jnp.int32, square, 0) < lax.broadcasted_iota(
            jnp.int32, square, 1
        )
        before = jnp.dot(
            named.astype(jnp.bfloat16),
            jnp.where(earlier, 1.0, 0.0).astype(jnp.bfloat16),
            preferred_element_type=jnp.float32,
        )
        slot = jnp.where(named > 0.0, before, -1.0)
        wide = (expert_count, row_count // expert_count, group_size)
        slot = jnp.broadcast_to(slot[:, None, :], wide).reshape(row_count, group_size)
        row = lax.broadcasted_iota(jnp.int32, (row_count, group_size), 0)
        wanted = part_ref[0] * SLOTS + jnp.bitwise_and(row, SLOTS - 1)
        onehot_ref[...] = jnp.where(slot == wanted.astype(jnp.float32), 1.0, 0.0).astype(
            jnp.bfloat16
        )

    out_ref[...] = jnp.dot(
        onehot_ref[...], tokens_ref[...], preferred_element_type=jnp.float32
    ).astype(jnp.bfloat16)


def packed_slots(moe_tokens, expert_ids, expert_count):
    group_size, width = moe_tokens.shape
    row_count = 2 * expert_count * SLOTS
    steps = 2
    part = (lax.axis_index("zl") * 2 + lax.axis_index("core")).astype(jnp.int32).reshape(1)
    packed = pl.pallas_call(
        pack_kernel,
        grid=(steps,),
        out_shape=jax.ShapeDtypeStruct((row_count, width), jnp.bfloat16),
        in_specs=[
            pl.BlockSpec(memory_space=pltpu.SMEM),
            pl.BlockSpec((2, group_size), lambda i: (0, 0)),
            pl.BlockSpec((group_size, width // steps), lambda i: (0, i)),
        ],
        out_specs=pl.BlockSpec((row_count, width // steps), lambda i: (0, i)),
        scratch_shapes=[pltpu.VMEM((row_count, group_size), jnp.bfloat16)],
        cost_estimate=pl.CostEstimate(
            flops=2 * row_count * group_size * width,
            bytes_accessed=2 * (row_count + group_size) * width,
            transcendentals=0,
        ),
        name="pack",
    )(part, expert_ids.T, moe_tokens)
    return packed.reshape(2 * expert_count, SLOTS, width)


def hidden_kernel(part_ref, slots_ref, head_ref, *refs):
    pieces, (out_ref, slots, weights, slots_sem, sems) = refs[:8], refs[8:]
    count = pieces[0].shape[0]
    head = head_ref.shape[0]
    copies = [pltpu.make_async_copy(slots_ref, slots, slots_sem)]
    for i, piece in enumerate(pieces):
        copies.append(
            pltpu.make_async_copy(piece, weights.at[pl.ds(i * count, count)], sems.at[i])
        )
    for copy in copies:
        copy.start()
    out_ref[pl.ds(0, head), :] = head_ref[...]
    copies[0].wait()
    part = part_ref[0]
    for first in range(0, 4, 2):
        for copy in copies[1 + 2 * first : 1 + 2 * (first + 2)]:
            copy.wait()
        sums = [
            lax.dot_general(
                weights[pl.ds(2 * count * member, 2 * count), :],
                slots[...],
                (((1,), (1,)), ((), ())),
                preferred_element_type=jnp.float32,
            )
            for member in range(first, first + 2)
        ]
        for i, both in enumerate(sums):
            gate, up = both[:count], both[count:]
            place = jnp.bitwise_xor(part, first + i) * count + head
            hidden = gate / (1.0 + jnp.exp(-gate)) * up
            out_ref[pl.ds(pl.multiple_of(place, 16), count), :] = hidden.astype(jnp.bfloat16)


def ring_message(arrived, head, gates, ups):
    count = gates[0].shape[1]
    slot_count, width = arrived.shape
    pieces = [weight.T for pair in zip(gates, ups) for weight in pair]
    part = (lax.axis_index("zl") * 2 + lax.axis_index("core")).astype(jnp.int32).reshape(1)
    anywhere = pl.BlockSpec(memory_space=pl.ANY)
    return pl.pallas_call(
        hidden_kernel,
        out_shape=jax.ShapeDtypeStruct((head.shape[0] + 4 * count, slot_count), jnp.bfloat16),
        in_specs=[
            pl.BlockSpec(memory_space=pltpu.SMEM),
            anywhere,
            pl.BlockSpec(memory_space=pltpu.VMEM),
            *[anywhere] * 8,
        ],
        out_specs=pl.BlockSpec(memory_space=pltpu.VMEM),
        scratch_shapes=[
            pltpu.VMEM((slot_count, width), jnp.bfloat16),
            pltpu.VMEM((8 * count, width), jnp.bfloat16),
            pltpu.SemaphoreType.DMA,
            pltpu.SemaphoreType.DMA((8,)),
        ],
        cost_estimate=pl.CostEstimate(
            flops=16 * count * slot_count * width,
            bytes_accessed=2 * (8 * count + slot_count) * width,
            transcendentals=4 * count * slot_count,
        ),
        name="hidden",
    )(part, arrived, head, *pieces)


def down_sums(message, head, down):
    place = lax.axis_index("zh")
    count = lax.axis_size("zh")
    size = message.shape[0] - head
    ahead = [(i, (i + 1) % count) for i in range(count)]
    behind = [(i, (i - 1) % count) for i in range(count)]

    def product(offset, first, shard):
        start = (place + (offset + count)) % count * size + first
        rows = lax.dynamic_slice_in_dim(down, start, shard.shape[0], 0)
        return lax.dot_general(
            shard, rows, (((0,), (0,)), ((), ())), preferred_element_type=jnp.float32
        )

    def both(step, near):
        return product(-step, 0, near[0][head:]) + product(step, 0, near[1][head:])

    forward = backward = message
    offsets, extras = [], []
    total = product(0, 0, message[head:])
    last = count // 2
    for step in range(1, last):
        forward = lax.ppermute(forward, "zh", ahead)
        backward = lax.ppermute(backward, "zh", behind)
        offsets += [-step, step]
        extras += [forward, backward]
        total = total + both(step, (forward, backward))
    half = (size + head) // 32 * 16
    forward = lax.ppermute(forward[:half], "zh", ahead)
    backward = lax.ppermute(backward[half:], "zh", behind)
    offsets.append(-last)
    extras.append(forward)
    total = total + product(-last, 0, forward[head:]) + product(last, half - head, backward)
    return total, offsets, extras


def ordered(blocks):
    for axis, dim in (("zl", 0), ("core", 1)):
        blocks = jnp.where(lax.axis_index(axis) == 0, blocks, jnp.flip(blocks, dim))
    return blocks


def layer(
    seq_inputs,
    step_size,
    write_map,
    read_map,
    decay_log,
    skip_gain,
    moe_tokens,
    expert_ids,
    route_weights,
    gate_proj,
    up_proj,
    down_proj,
):
    group_size = moe_tokens.shape[0]
    expert_count = lax.axis_size("exp") // 2
    capacity = min(group_size, 4 * group_size // expert_count)
    rows = SLOTS
    assert capacity == 4 * rows
    gate, up, down = gate_proj[0], up_proj[0], down_proj[0]
    gate_across = swap(gate, "zl")
    packed = packed_slots(moe_tokens, expert_ids, expert_count)
    packed, gate, up, down, seq_inputs, step_size = lax.optimization_barrier(
        (packed, gate, up, down, seq_inputs, step_size)
    )
    arrived = lax.all_to_all(packed, "exp", split_axis=0, concat_axis=0, tiled=True)
    up_across = swap(up, "zl")
    down_across = swap(down, "zl")
    gates = four(gate, gate_across)
    ups = four(up, up_across)
    down_columns = jnp.concatenate(four(down, down_across), axis=1)
    local_mix, cumulative, block_ends, entering, final = mixer_prepare(
        seq_inputs, step_size, write_map, read_map, decay_log
    )
    group, before = group_state(jnp.sum(block_ends, axis=1), final)
    state_part = state_rows(*group, 2 * expert_count * rows)
    head = state_part.shape[0]
    message = ring_message(
        arrived.reshape(2 * expert_count * rows, -1), state_part, gates, ups
    )
    sums, offsets, extras = down_sums(message, head, down_columns)
    width = down.shape[1]
    blocks = sums.reshape(2 * expert_count, rows, 4, width).transpose(2, 0, 1, 3)
    blocks = ordered(blocks.reshape(2, 2, 2 * expert_count, rows, width))
    blocks = blocks.transpose(2, 0, 1, 3, 4).reshape(8 * expert_count, rows, width)
    blocks, expert_ids, route_weights, *extras = lax.optimization_barrier(
        (blocks, expert_ids, route_weights, *extras)
    )
    returned = lax.all_to_all(
        blocks, ("exp", "zl", "core"), split_axis=0, concat_axis=0, tiled=True
    )
    states = jnp.stack([message[:head] for message in extras])
    state_before = state_ahead(offsets, *read_rows(states, final.shape), before)
    mixer_output = mixer_finish(
        local_mix, cumulative, block_ends, entering, state_before, read_map, seq_inputs, skip_gain
    )
    combine = combine_map(expert_ids, route_weights, expert_count, capacity)
    summed = jnp.sum(returned.reshape(expert_count, 2, capacity, width), axis=1)
    expert_output = jnp.dot(
        combine,
        summed.reshape(expert_count * capacity, width),
        precision=HIGHEST,
        preferred_element_type=jnp.float32,
    ).astype(jnp.bfloat16)
    return (mixer_output, expert_output)


def solution(mesh):
    devices = mesh.devices
    ctx_size, exp_size = devices.shape
    split = jax.sharding.Mesh(
        devices.reshape(ctx_size // 4, 2, 2, exp_size), ("zh", "zl", "core", "exp")
    )
    return jax.shard_map(
        layer,
        mesh=split,
        in_specs=(
            P(CTX, "exp"),
            P("exp", CTX),
            P(None, CTX),
            P(None, CTX),
            P("exp"),
            P("exp"),
            P("exp", None),
            P("exp", None),
            P("exp", None),
            P("exp", None, CTX),
            P("exp", None, CTX),
            P("exp", None, CTX),
        ),
        out_specs=(P(CTX, "exp"), P("exp", CTX)),
        check_vma=False,
    )
```

```python
import jax
import jax.numpy as jnp
from jax import lax
from jax.experimental import pallas as pl
from jax.experimental.pallas import tpu as pltpu
from jax.sharding import PartitionSpec as P

BLOCK = 256


HIGHEST = lax.Precision.HIGHEST


def block_chain(running, pieces):
    decay, increment = pieces
    return (decay[:, None, None] * running + increment, running)


def mixer_prepare(seq_inputs, step_size, write_map, read_map, decay_log):
    length = seq_inputs.shape[0]
    head_count = step_size.shape[0]
    state_count = write_map.shape[0]
    head_width = seq_inputs.shape[1] // head_count
    block_count = length // BLOCK
    decay_rate = -jnp.exp(decay_log)
    log_decay = (step_size * decay_rate[:, None]).reshape(head_count, block_count, BLOCK)
    cumulative = jnp.cumsum(log_decay, axis=2)
    block_ends = cumulative[:, :, BLOCK - 1]
    step_blocks = step_size.reshape(head_count, block_count, BLOCK)
    write_blocks = write_map.reshape(state_count, block_count, BLOCK)
    read_blocks = read_map.reshape(state_count, block_count, BLOCK)
    value_blocks = seq_inputs.reshape(block_count, BLOCK, head_count, head_width)
    scores = jnp.einsum(
        "nkt,nks->kts", read_blocks, write_blocks, preferred_element_type=jnp.float32
    )
    row_index = lax.broadcasted_iota(jnp.int32, (BLOCK, BLOCK), 0)
    column_index = lax.broadcasted_iota(jnp.int32, (BLOCK, BLOCK), 1)
    lower = column_index <= row_index
    difference = cumulative[:, :, :, None] - cumulative[:, :, None, :]
    decay = jnp.where(lower[None, None], jnp.exp(jnp.minimum(difference, 0.0)), 0.0)
    mixing = (scores[None] * decay * step_blocks[:, :, None, :]).astype(jnp.bfloat16)
    local_mix = jnp.einsum(
        "hkts,kshp->kthp", mixing, value_blocks, preferred_element_type=jnp.float32
    )
    weights = jnp.exp(block_ends[:, :, None] - cumulative) * step_blocks
    key_decayed = (write_blocks[None] * weights[:, None]).astype(jnp.bfloat16)
    increments = jnp.einsum(
        "hnks,kshp->khnp", key_decayed, value_blocks, preferred_element_type=jnp.float32
    )
    zero_state = jnp.zeros((head_count, state_count, head_width), jnp.float32)
    final, entering = lax.scan(block_chain, zero_state, (jnp.exp(block_ends).T, increments))
    return (local_mix, cumulative, block_ends, entering, final)


def mixer_finish(
    local_mix, cumulative, block_ends, entering, state_before, read_map, seq_inputs, skip_gain
):
    head_count = block_ends.shape[0]
    block_count = block_ends.shape[1]
    state_count = read_map.shape[0]
    head_width = entering.shape[3]
    before = jnp.cumsum(block_ends, axis=1) - block_ends
    states = jnp.exp(before).T[:, :, None, None] * state_before[None] + entering
    read_blocks = read_map.reshape(state_count, block_count, BLOCK).astype(jnp.float32)
    carried = jnp.einsum("nkt,khnp->kthp", read_blocks, states, precision=HIGHEST)
    carried = carried * jnp.exp(cumulative).transpose(1, 2, 0)[:, :, :, None]
    value_blocks = seq_inputs.reshape(block_count, BLOCK, head_count, head_width).astype(
        jnp.float32
    )
    output = local_mix + carried + skip_gain[None, None, :, None] * value_blocks
    return output.reshape(seq_inputs.shape).astype(jnp.bfloat16)


CTX = ("zh", "zl", "core")
SWAP = ((0, 1), (1, 0))
SLOTS = 8


def swap(array, axis):
    return lax.ppermute(array, axis, SWAP)


def four(array, across):
    beside = swap(array, "core")
    return (array, beside, across, swap(across, "core"))


def joined(first, second):
    return first[0] + second[0], jnp.exp(second[0])[:, None, None] * first[1] + second[1]


def exchanged(pair, axis):
    log, state = pair
    both = jnp.concatenate([log[:, None], state.reshape(state.shape[0], -1)], axis=1)
    received = swap(both, axis)
    return received[:, 0], received[:, 1:].reshape(state.shape)


def chosen(flag, left, right):
    return jax.tree.map(lambda a, b: jnp.where(flag, a, b), left, right)


def group_state(total_log, final):
    own = (total_log, final)
    before = jax.tree.map(jnp.zeros_like, own)
    for axis in ("core", "zl"):
        other = exchanged(own, axis)
        later = lax.axis_index(axis) == 1
        before = chosen(later, joined(other, before), before)
        own = chosen(later, joined(other, own), joined(own, other))
    return own, before


def upper(array):
    return lax.reduce_precision(array, 8, 7)


def state_rows(log, state, width):
    flat = state.reshape(-1, width)
    high = upper(flat)
    first = upper(log)
    second = upper(log - first)
    logs = jnp.stack([first, second, log - first - second])
    logs = jnp.pad(logs, ((0, flat.shape[0] - 3), (0, width - log.shape[0])))
    return jnp.concatenate([high, flat - high, logs], axis=0).astype(jnp.bfloat16)


def read_rows(rows, shape):
    count, _, width = rows.shape
    parts = rows.reshape(count, 3, -1, width).astype(jnp.float32)
    logs = jnp.sum(parts[:, 2, :3, : shape[0]], axis=1)
    return logs, (parts[:, 0] + parts[:, 1]).reshape(count, *shape)


def state_ahead(offsets, logs, states, before):
    place = lax.axis_index("zh")
    count = lax.axis_size("zh")
    sign = 1 - 2 * lax.axis_index("core")
    source = jnp.bitwise_and(place + sign * jnp.array(offsets, jnp.int32) + count, count - 1)
    earlier = source < place
    between = (source[None, :] > source[:, None]) & earlier[None, :]
    span = jnp.sum(jnp.where(between[:, :, None], logs[None], 0.0), axis=1)
    factor = jnp.where(earlier[:, None], jnp.exp(span), 0.0)
    outside = jnp.sum(factor[:, :, None, None] * states, axis=0)
    return joined((jnp.zeros_like(before[0]), outside), before)[1]


def combine_map(expert_ids, route_weights, expert_count, capacity):
    group_size = expert_ids.shape[0]
    assigned = expert_ids.reshape(group_size * 2)
    onehot = (
        assigned[:, None] == lax.broadcasted_iota(jnp.int32, (group_size * 2, expert_count), 1)
    ).astype(jnp.int32)
    earlier_count = jnp.cumsum(onehot, axis=0) - onehot
    position = jnp.sum((earlier_count + assigned[:, None] * capacity) * onehot, axis=1)
    matches = (
        position[:, None]
        == lax.broadcasted_iota(jnp.int32, (group_size * 2, expert_count * capacity), 1)
    ).astype(jnp.float32)
    return jnp.sum(
        (matches * route_weights.reshape(group_size * 2)[:, None]).reshape(group_size, 2, -1),
        axis=1,
    )


def pack_kernel(part_ref, ids_ref, tokens_ref, out_ref, onehot_ref):
    group_size = tokens_ref.shape[0]
    row_count = out_ref.shape[0]
    expert_count = row_count // (2 * SLOTS)

    @pl.when(pl.program_id(0) == 0)
    def _():
        shape = (expert_count, group_size)
        expert = lax.broadcasted_iota(jnp.int32, shape, 0)
        named = (ids_ref[0:1, :] == expert) | (ids_ref[1:2, :] == expert)
        named = jnp.where(named, 1.0, 0.0)
        square = (group_size, group_size)
        earlier = lax.broadcasted_iota(jnp.int32, square, 0) < lax.broadcasted_iota(
            jnp.int32, square, 1
        )
        before = jnp.dot(
            named.astype(jnp.bfloat16),
            jnp.where(earlier, 1.0, 0.0).astype(jnp.bfloat16),
            preferred_element_type=jnp.float32,
        )
        slot = jnp.where(named > 0.0, before, -1.0)
        wide = (expert_count, row_count // expert_count, group_size)
        slot = jnp.broadcast_to(slot[:, None, :], wide).reshape(row_count, group_size)
        row = lax.broadcasted_iota(jnp.int32, (row_count, group_size), 0)
        wanted = part_ref[0] * SLOTS + jnp.bitwise_and(row, SLOTS - 1)
        onehot_ref[...] = jnp.where(slot == wanted.astype(jnp.float32), 1.0, 0.0).astype(
            jnp.bfloat16
        )

    out_ref[...] = jnp.dot(
        onehot_ref[...], tokens_ref[...], preferred_element_type=jnp.float32
    ).astype(jnp.bfloat16)


def packed_slots(moe_tokens, expert_ids, expert_count):
    group_size, width = moe_tokens.shape
    row_count = 2 * expert_count * SLOTS
    steps = 2
    part = (lax.axis_index("zl") * 2 + lax.axis_index("core")).astype(jnp.int32).reshape(1)
    packed = pl.pallas_call(
        pack_kernel,
        grid=(steps,),
        out_shape=jax.ShapeDtypeStruct((row_count, width), jnp.bfloat16),
        in_specs=[
            pl.BlockSpec(memory_space=pltpu.SMEM),
            pl.BlockSpec((2, group_size), lambda i: (0, 0)),
            pl.BlockSpec((group_size, width // steps), lambda i: (0, i)),
        ],
        out_specs=pl.BlockSpec((row_count, width // steps), lambda i: (0, i)),
        scratch_shapes=[pltpu.VMEM((row_count, group_size), jnp.bfloat16)],
        cost_estimate=pl.CostEstimate(
            flops=2 * row_count * group_size * width,
            bytes_accessed=2 * (row_count + group_size) * width,
            transcendentals=0,
        ),
        name="pack",
    )(part, expert_ids.T, moe_tokens)
    return packed.reshape(2 * expert_count, SLOTS, width)


def hidden_kernel(part_ref, slots_ref, head_ref, *refs):
    pieces, (out_ref, slots, weights, slots_sem, sems) = refs[:8], refs[8:]
    count = pieces[0].shape[0]
    head = head_ref.shape[0]
    copies = [pltpu.make_async_copy(slots_ref, slots, slots_sem)]
    for i, piece in enumerate(pieces):
        copies.append(
            pltpu.make_async_copy(piece, weights.at[pl.ds(i * count, count)], sems.at[i])
        )
    for copy in copies:
        copy.start()
    out_ref[pl.ds(0, head), :] = head_ref[...]
    copies[0].wait()
    part = part_ref[0]
    for first in range(0, 4, 2):
        for copy in copies[1 + 2 * first : 1 + 2 * (first + 2)]:
            copy.wait()
        sums = [
            lax.dot_general(
                weights[pl.ds(2 * count * member, 2 * count), :],
                slots[...],
                (((1,), (1,)), ((), ())),
                preferred_element_type=jnp.float32,
            )
            for member in range(first, first + 2)
        ]
        for i, both in enumerate(sums):
            gate, up = both[:count], both[count:]
            place = jnp.bitwise_xor(part, first + i) * count + head
            hidden = gate / (1.0 + jnp.exp(-gate)) * up
            out_ref[pl.ds(pl.multiple_of(place, 16), count), :] = hidden.astype(jnp.bfloat16)


def ring_message(arrived, head, gates, ups):
    count = gates[0].shape[1]
    slot_count, width = arrived.shape
    pieces = [weight.T for pair in zip(gates, ups) for weight in pair]
    part = (lax.axis_index("zl") * 2 + lax.axis_index("core")).astype(jnp.int32).reshape(1)
    anywhere = pl.BlockSpec(memory_space=pl.ANY)
    return pl.pallas_call(
        hidden_kernel,
        out_shape=jax.ShapeDtypeStruct((head.shape[0] + 4 * count, slot_count), jnp.bfloat16),
        in_specs=[
            pl.BlockSpec(memory_space=pltpu.SMEM),
            anywhere,
            pl.BlockSpec(memory_space=pltpu.VMEM),
            *[anywhere] * 8,
        ],
        out_specs=pl.BlockSpec(memory_space=pltpu.VMEM),
        scratch_shapes=[
            pltpu.VMEM((slot_count, width), jnp.bfloat16),
            pltpu.VMEM((8 * count, width), jnp.bfloat16),
            pltpu.SemaphoreType.DMA,
            pltpu.SemaphoreType.DMA((8,)),
        ],
        cost_estimate=pl.CostEstimate(
            flops=16 * count * slot_count * width,
            bytes_accessed=2 * (8 * count + slot_count) * width,
            transcendentals=4 * count * slot_count,
        ),
        name="hidden",
    )(part, arrived, head, *pieces)


def down_sums(message, head, downs):
    place = lax.axis_index("zh")
    count = lax.axis_size("zh")
    size = message.shape[0] - head
    sign = 1 - 2 * lax.axis_index("core")

    def pairs(way):
        steps = (way, -way)
        return [
            (2 * i + core, 2 * ((i + steps[core]) % count) + core)
            for i in range(count)
            for core in range(2)
        ]

    def move(array, way):
        return lax.ppermute(array, ("zh", "core"), pairs(way))

    def product(offset, first, shard):
        start = jnp.bitwise_and(place + sign * offset + count, count - 1) * size + first
        return [
            lax.dot_general(
                shard,
                lax.dynamic_slice_in_dim(down, start, shard.shape[0], 0),
                (((0,), (0,)), ((), ())),
                preferred_element_type=jnp.float32,
            )
            for down in downs
        ]

    def added(*parts):
        return [sum(part[1:], part[0]) for part in zip(*parts)]

    first = second = message
    offsets, received = [], []
    total = product(0, 0, message[head:])
    last = count // 2
    for step in range(1, last):
        first = move(first, 1)
        second = move(second, -1)
        offsets += [-step, step]
        received += [first, second]
        total = added(total, product(-step, 0, first[head:]), product(step, 0, second[head:]))
    half = (size + head) // 32 * 16
    first = move(first[:half], 1)
    second = move(second[half:], -1)
    offsets.append(-last)
    received.append(first)
    total = added(
        total, product(-last, 0, first[head:]), product(last, half - head, second)
    )
    return total, offsets, received


def ordered(blocks):
    for axis, dim in (("zl", 0), ("core", 1)):
        blocks = jnp.where(lax.axis_index(axis) == 0, blocks, jnp.flip(blocks, dim))
    return blocks


def layer(
    seq_inputs,
    step_size,
    write_map,
    read_map,
    decay_log,
    skip_gain,
    moe_tokens,
    expert_ids,
    route_weights,
    gate_proj,
    up_proj,
    down_proj,
):
    group_size = moe_tokens.shape[0]
    expert_count = lax.axis_size("exp") // 2
    capacity = min(group_size, 4 * group_size // expert_count)
    rows = SLOTS
    assert capacity == 4 * rows
    gate, up, down = gate_proj[0], up_proj[0], down_proj[0]
    gate_across = swap(gate, "zl")
    packed = packed_slots(moe_tokens, expert_ids, expert_count)
    packed, gate, up, down, seq_inputs, step_size = lax.optimization_barrier(
        (packed, gate, up, down, seq_inputs, step_size)
    )
    arrived = lax.all_to_all(packed, "exp", split_axis=0, concat_axis=0, tiled=True)
    up_across = swap(up, "zl")
    down_across = swap(down, "zl")
    gates = four(gate, gate_across)
    ups = four(up, up_across)
    downs = four(down, down_across)
    near = jnp.concatenate(downs[:2], axis=1)
    downs = near, jnp.concatenate(downs[2:], axis=1)
    local_mix, cumulative, block_ends, entering, final = mixer_prepare(
        seq_inputs, step_size, write_map, read_map, decay_log
    )
    group, before = group_state(jnp.sum(block_ends, axis=1), final)
    state_part = state_rows(*group, 2 * expert_count * rows)
    head = state_part.shape[0]
    message = ring_message(
        arrived.reshape(2 * expert_count * rows, -1), state_part, gates, ups
    )
    sums, offsets, extras = down_sums(message, head, downs)
    width = down.shape[1]
    blocks = jnp.stack(
        [part.reshape(2 * expert_count, rows, 2, width).transpose(2, 0, 1, 3) for part in sums]
    )
    blocks = ordered(blocks)
    blocks = blocks.transpose(2, 0, 1, 3, 4).reshape(8 * expert_count, rows, width)
    blocks, expert_ids, route_weights, *extras = lax.optimization_barrier(
        (blocks, expert_ids, route_weights, *extras)
    )
    returned = lax.all_to_all(
        blocks, ("exp", "zl", "core"), split_axis=0, concat_axis=0, tiled=True
    )
    states = jnp.stack([message[:head] for message in extras])
    state_before = state_ahead(offsets, *read_rows(states, final.shape), before)
    mixer_output = mixer_finish(
        local_mix, cumulative, block_ends, entering, state_before, read_map, seq_inputs, skip_gain
    )
    combine = combine_map(expert_ids, route_weights, expert_count, capacity)
    summed = jnp.sum(returned.reshape(expert_count, 2, capacity, width), axis=1)
    expert_output = jnp.dot(
        combine,
        summed.reshape(expert_count * capacity, width),
        precision=HIGHEST,
        preferred_element_type=jnp.float32,
    ).astype(jnp.bfloat16)
    return (mixer_output, expert_output)


def solution(mesh):
    devices = mesh.devices
    ctx_size, exp_size = devices.shape
    split = jax.sharding.Mesh(
        devices.reshape(ctx_size // 4, 2, 2, exp_size), ("zh", "zl", "core", "exp")
    )
    return jax.shard_map(
        layer,
        mesh=split,
        in_specs=(
            P(CTX, "exp"),
            P("exp", CTX),
            P(None, CTX),
            P(None, CTX),
            P("exp"),
            P("exp"),
            P("exp", None),
            P("exp", None),
            P("exp", None),
            P("exp", None, CTX),
            P("exp", None, CTX),
            P("exp", None, CTX),
        ),
        out_specs=(P(CTX, "exp"), P("exp", CTX)),
        check_vma=False,
    )
```

```python
import jax
import jax.numpy as jnp
from jax import lax
from jax.experimental import pallas as pl
from jax.experimental.pallas import tpu as pltpu
from jax.sharding import PartitionSpec as P

BLOCK = 256


HIGHEST = lax.Precision.HIGHEST


def block_chain(running, pieces):
    decay, increment = pieces
    return (decay[:, None, None] * running + increment, running)


def mixer_prepare(seq_inputs, step_size, write_map, read_map, decay_log):
    length = seq_inputs.shape[0]
    head_count = step_size.shape[0]
    state_count = write_map.shape[0]
    head_width = seq_inputs.shape[1] // head_count
    block_count = length // BLOCK
    decay_rate = -jnp.exp(decay_log)
    log_decay = (step_size * decay_rate[:, None]).reshape(head_count, block_count, BLOCK)
    cumulative = jnp.cumsum(log_decay, axis=2)
    block_ends = cumulative[:, :, BLOCK - 1]
    step_blocks = step_size.reshape(head_count, block_count, BLOCK)
    write_blocks = write_map.reshape(state_count, block_count, BLOCK)
    read_blocks = read_map.reshape(state_count, block_count, BLOCK)
    value_blocks = seq_inputs.reshape(block_count, BLOCK, head_count, head_width)
    scores = jnp.einsum(
        "nkt,nks->kts", read_blocks, write_blocks, preferred_element_type=jnp.float32
    )
    row_index = lax.broadcasted_iota(jnp.int32, (BLOCK, BLOCK), 0)
    column_index = lax.broadcasted_iota(jnp.int32, (BLOCK, BLOCK), 1)
    lower = column_index <= row_index
    difference = cumulative[:, :, :, None] - cumulative[:, :, None, :]
    decay = jnp.where(lower[None, None], jnp.exp(jnp.minimum(difference, 0.0)), 0.0)
    mixing = (scores[None] * decay * step_blocks[:, :, None, :]).astype(jnp.bfloat16)
    local_mix = jnp.einsum(
        "hkts,kshp->kthp", mixing, value_blocks, preferred_element_type=jnp.float32
    )
    weights = jnp.exp(block_ends[:, :, None] - cumulative) * step_blocks
    key_decayed = (write_blocks[None] * weights[:, None]).astype(jnp.bfloat16)
    increments = jnp.einsum(
        "hnks,kshp->khnp", key_decayed, value_blocks, preferred_element_type=jnp.float32
    )
    zero_state = jnp.zeros((head_count, state_count, head_width), jnp.float32)
    final, entering = lax.scan(block_chain, zero_state, (jnp.exp(block_ends).T, increments))
    return (local_mix, cumulative, block_ends, entering, final)


def mixer_finish(
    local_mix, cumulative, block_ends, entering, state_before, read_map, seq_inputs, skip_gain
):
    head_count = block_ends.shape[0]
    block_count = block_ends.shape[1]
    state_count = read_map.shape[0]
    head_width = entering.shape[3]
    before = jnp.cumsum(block_ends, axis=1) - block_ends
    states = jnp.exp(before).T[:, :, None, None] * state_before[None] + entering
    read_blocks = read_map.reshape(state_count, block_count, BLOCK).astype(jnp.float32)
    carried = jnp.einsum("nkt,khnp->kthp", read_blocks, states, precision=HIGHEST)
    carried = carried * jnp.exp(cumulative).transpose(1, 2, 0)[:, :, :, None]
    value_blocks = seq_inputs.reshape(block_count, BLOCK, head_count, head_width).astype(
        jnp.float32
    )
    output = local_mix + carried + skip_gain[None, None, :, None] * value_blocks
    return output.reshape(seq_inputs.shape).astype(jnp.bfloat16)


CTX = ("zh", "zl", "core")
SWAP = ((0, 1), (1, 0))
SLOTS = 8


def swap(array, axis):
    return lax.ppermute(array, axis, SWAP)


def four(array, across):
    beside = swap(array, "core")
    return (array, beside, across, swap(across, "core"))


def joined(first, second):
    return first[0] + second[0], jnp.exp(second[0])[:, None, None] * first[1] + second[1]


def exchanged(pair, axis):
    log, state = pair
    both = jnp.concatenate([log[:, None], state.reshape(state.shape[0], -1)], axis=1)
    received = swap(both, axis)
    return received[:, 0], received[:, 1:].reshape(state.shape)


def chosen(flag, left, right):
    return jax.tree.map(lambda a, b: jnp.where(flag, a, b), left, right)


def group_state(total_log, final):
    own = (total_log, final)
    before = jax.tree.map(jnp.zeros_like, own)
    for axis in ("core", "zl"):
        other = exchanged(own, axis)
        later = lax.axis_index(axis) == 1
        before = chosen(later, joined(other, before), before)
        own = chosen(later, joined(other, own), joined(own, other))
    return own, before


def upper(array):
    return lax.reduce_precision(array, 8, 7)


def state_rows(log, state, width):
    flat = state.reshape(-1, width)
    high = upper(flat)
    first = upper(log)
    second = upper(log - first)
    logs = jnp.stack([first, second, log - first - second])
    logs = jnp.pad(logs, ((0, flat.shape[0] - 3), (0, width - log.shape[0])))
    return jnp.concatenate([high, flat - high, logs], axis=0).astype(jnp.bfloat16)


def read_rows(rows, shape):
    count, _, width = rows.shape
    parts = rows.reshape(count, 3, -1, width).astype(jnp.float32)
    logs = jnp.sum(parts[:, 2, :3, : shape[0]], axis=1)
    return logs, (parts[:, 0] + parts[:, 1]).reshape(count, *shape)


def state_ahead(offsets, logs, states, before):
    place = lax.axis_index("zh")
    count = lax.axis_size("zh")
    sign = 1 - 2 * lax.axis_index("core")
    source = jnp.bitwise_and(place + sign * jnp.array(offsets, jnp.int32) + count, count - 1)
    earlier = source < place
    between = (source[None, :] > source[:, None]) & earlier[None, :]
    span = jnp.sum(jnp.where(between[:, :, None], logs[None], 0.0), axis=1)
    factor = jnp.where(earlier[:, None], jnp.exp(span), 0.0)
    outside = jnp.sum(factor[:, :, None, None] * states, axis=0)
    return joined((jnp.zeros_like(before[0]), outside), before)[1]


def combine_map(expert_ids, route_weights, expert_count, capacity):
    group_size = expert_ids.shape[0]
    assigned = expert_ids.reshape(group_size * 2)
    onehot = (
        assigned[:, None] == lax.broadcasted_iota(jnp.int32, (group_size * 2, expert_count), 1)
    ).astype(jnp.int32)
    earlier_count = jnp.cumsum(onehot, axis=0) - onehot
    position = jnp.sum((earlier_count + assigned[:, None] * capacity) * onehot, axis=1)
    matches = (
        position[:, None]
        == lax.broadcasted_iota(jnp.int32, (group_size * 2, expert_count * capacity), 1)
    ).astype(jnp.float32)
    return jnp.sum(
        (matches * route_weights.reshape(group_size * 2)[:, None]).reshape(group_size, 2, -1),
        axis=1,
    )


def pack_kernel(part_ref, ids_ref, tokens_ref, out_ref, onehot_ref):
    group_size = tokens_ref.shape[0]
    row_count = out_ref.shape[0]
    expert_count = row_count // (2 * SLOTS)

    @pl.when(pl.program_id(0) == 0)
    def _():
        shape = (expert_count, group_size)
        expert = lax.broadcasted_iota(jnp.int32, shape, 0)
        named = (ids_ref[0:1, :] == expert) | (ids_ref[1:2, :] == expert)
        named = jnp.where(named, 1.0, 0.0)
        square = (group_size, group_size)
        earlier = lax.broadcasted_iota(jnp.int32, square, 0) < lax.broadcasted_iota(
            jnp.int32, square, 1
        )
        before = jnp.dot(
            named.astype(jnp.bfloat16),
            jnp.where(earlier, 1.0, 0.0).astype(jnp.bfloat16),
            preferred_element_type=jnp.float32,
        )
        slot = jnp.where(named > 0.0, before, -1.0)
        wide = (expert_count, row_count // expert_count, group_size)
        slot = jnp.broadcast_to(slot[:, None, :], wide).reshape(row_count, group_size)
        row = lax.broadcasted_iota(jnp.int32, (row_count, group_size), 0)
        wanted = part_ref[0] * SLOTS + jnp.bitwise_and(row, SLOTS - 1)
        onehot_ref[...] = jnp.where(slot == wanted.astype(jnp.float32), 1.0, 0.0).astype(
            jnp.bfloat16
        )

    out_ref[...] = jnp.dot(
        onehot_ref[...], tokens_ref[...], preferred_element_type=jnp.float32
    ).astype(jnp.bfloat16)


def packed_slots(moe_tokens, expert_ids, expert_count):
    group_size, width = moe_tokens.shape
    row_count = 2 * expert_count * SLOTS
    steps = 2
    part = (lax.axis_index("zl") * 2 + lax.axis_index("core")).astype(jnp.int32).reshape(1)
    packed = pl.pallas_call(
        pack_kernel,
        grid=(steps,),
        out_shape=jax.ShapeDtypeStruct((row_count, width), jnp.bfloat16),
        in_specs=[
            pl.BlockSpec(memory_space=pltpu.SMEM),
            pl.BlockSpec((2, group_size), lambda i: (0, 0)),
            pl.BlockSpec((group_size, width // steps), lambda i: (0, i)),
        ],
        out_specs=pl.BlockSpec((row_count, width // steps), lambda i: (0, i)),
        scratch_shapes=[pltpu.VMEM((row_count, group_size), jnp.bfloat16)],
        cost_estimate=pl.CostEstimate(
            flops=2 * row_count * group_size * width,
            bytes_accessed=2 * (row_count + group_size) * width,
            transcendentals=0,
        ),
        name="pack",
    )(part, expert_ids.T, moe_tokens)
    return packed.reshape(2 * expert_count, SLOTS, width)


def hidden_kernel(part_ref, slots_ref, head_ref, *refs):
    pieces, (out_ref, weights, sems) = refs[:8], refs[8:]
    count = pieces[0].shape[0]
    head = head_ref.shape[0]
    copies = []
    for i, piece in enumerate(pieces):
        copies.append(
            pltpu.make_async_copy(piece, weights.at[pl.ds(i * count, count)], sems.at[i])
        )
    for copy in copies:
        copy.start()
    out_ref[pl.ds(0, head), :] = head_ref[...]
    part = part_ref[0]
    for first in range(0, 4, 2):
        for copy in copies[2 * first : 2 * (first + 2)]:
            copy.wait()
        sums = [
            lax.dot_general(
                weights[pl.ds(2 * count * member, 2 * count), :],
                slots_ref[...],
                (((1,), (1,)), ((), ())),
                preferred_element_type=jnp.float32,
            )
            for member in range(first, first + 2)
        ]
        for i, both in enumerate(sums):
            gate, up = both[:count], both[count:]
            place = jnp.bitwise_xor(part, first + i) * count + head
            hidden = gate / (1.0 + jnp.exp(-gate)) * up
            out_ref[pl.ds(pl.multiple_of(place, 16), count), :] = hidden.astype(jnp.bfloat16)


def ring_message(arrived, head, gates, ups):
    count = gates[0].shape[1]
    slot_count, width = arrived.shape
    pieces = [
        pltpu.with_memory_space_constraint(weight.T, pltpu.HBM)
        for pair in zip(gates, ups)
        for weight in pair
    ]
    part = (lax.axis_index("zl") * 2 + lax.axis_index("core")).astype(jnp.int32).reshape(1)
    anywhere = pl.BlockSpec(memory_space=pl.ANY)
    inside = pl.BlockSpec(memory_space=pltpu.VMEM)
    arrived = pltpu.with_memory_space_constraint(arrived, pltpu.VMEM)
    return pl.pallas_call(
        hidden_kernel,
        out_shape=jax.ShapeDtypeStruct((head.shape[0] + 4 * count, slot_count), jnp.bfloat16),
        in_specs=[
            pl.BlockSpec(memory_space=pltpu.SMEM),
            inside,
            inside,
            *[anywhere] * 8,
        ],
        out_specs=inside,
        scratch_shapes=[
            pltpu.VMEM((8 * count, width), jnp.bfloat16),
            pltpu.SemaphoreType.DMA((8,)),
        ],
        cost_estimate=pl.CostEstimate(
            flops=16 * count * slot_count * width,
            bytes_accessed=2 * (8 * count + slot_count) * width,
            transcendentals=4 * count * slot_count,
        ),
        compiler_params=pltpu.CompilerParams(vmem_limit_bytes=24 * 2**20),
        name="hidden",
    )(part, arrived, head, *pieces)


def down_sums(message, head, downs):
    place = lax.axis_index("zh")
    count = lax.axis_size("zh")
    size = message.shape[0] - head
    sign = 1 - 2 * lax.axis_index("core")

    def pairs(way):
        steps = (way, -way)
        return [
            (2 * i + core, 2 * ((i + steps[core]) % count) + core)
            for i in range(count)
            for core in range(2)
        ]

    def move(array, way):
        return lax.ppermute(array, ("zh", "core"), pairs(way))

    def product(offset, first, shard):
        start = jnp.bitwise_and(place + sign * offset + count, count - 1) * size + first
        return [
            lax.dot_general(
                shard,
                lax.dynamic_slice_in_dim(down, start, shard.shape[0], 0),
                (((0,), (0,)), ((), ())),
                preferred_element_type=jnp.float32,
            )
            for down in downs
        ]

    def added(*parts):
        return [sum(part[1:], part[0]) for part in zip(*parts)]

    first = second = message
    offsets, received = [], []
    total = product(0, 0, message[head:])
    last = count // 2
    for step in range(1, last):
        first = move(first, 1)
        second = move(second, -1)
        offsets += [-step, step]
        received += [first, second]
        total = added(total, product(-step, 0, first[head:]), product(step, 0, second[head:]))
    half = (size + head) // 32 * 16
    first = move(first[:half], 1)
    second = move(second[half:], -1)
    offsets.append(-last)
    received.append(first)
    total = added(
        total, product(-last, 0, first[head:]), product(last, half - head, second)
    )
    return total, offsets, received


def ordered(blocks):
    for axis, dim in (("zl", 0), ("core", 1)):
        blocks = jnp.where(lax.axis_index(axis) == 0, blocks, jnp.flip(blocks, dim))
    return blocks


def layer(
    seq_inputs,
    step_size,
    write_map,
    read_map,
    decay_log,
    skip_gain,
    moe_tokens,
    expert_ids,
    route_weights,
    gate_proj,
    up_proj,
    down_proj,
):
    group_size = moe_tokens.shape[0]
    expert_count = lax.axis_size("exp") // 2
    capacity = min(group_size, 4 * group_size // expert_count)
    rows = SLOTS
    assert capacity == 4 * rows
    gate, up, down = gate_proj[0], up_proj[0], down_proj[0]
    gate_across = swap(gate, "zl")
    packed = packed_slots(moe_tokens, expert_ids, expert_count)
    packed, gate, up, down, seq_inputs, step_size = lax.optimization_barrier(
        (packed, gate, up, down, seq_inputs, step_size)
    )
    arrived = lax.all_to_all(packed, "exp", split_axis=0, concat_axis=0, tiled=True)
    up_across = swap(up, "zl")
    down_across = swap(down, "zl")
    gates = four(gate, gate_across)
    ups = four(up, up_across)
    downs = four(down, down_across)
    near = jnp.concatenate(downs[:2], axis=1)
    downs = near, jnp.concatenate(downs[2:], axis=1)
    local_mix, cumulative, block_ends, entering, final = mixer_prepare(
        seq_inputs, step_size, write_map, read_map, decay_log
    )
    group, before = group_state(jnp.sum(block_ends, axis=1), final)
    state_part = state_rows(*group, 2 * expert_count * rows)
    head = state_part.shape[0]
    message = ring_message(
        arrived.reshape(2 * expert_count * rows, -1), state_part, gates, ups
    )
    sums, offsets, extras = down_sums(message, head, downs)
    width = down.shape[1]
    blocks = jnp.stack(
        [part.reshape(2 * expert_count, rows, 2, width).transpose(2, 0, 1, 3) for part in sums]
    )
    blocks = ordered(blocks)
    blocks = blocks.transpose(2, 0, 1, 3, 4).reshape(8 * expert_count, rows, width)
    blocks, expert_ids, route_weights, *extras = lax.optimization_barrier(
        (blocks, expert_ids, route_weights, *extras)
    )
    returned = lax.all_to_all(
        blocks, ("exp", "zl", "core"), split_axis=0, concat_axis=0, tiled=True
    )
    states = jnp.stack([message[:head] for message in extras])
    state_before = state_ahead(offsets, *read_rows(states, final.shape), before)
    mixer_output = mixer_finish(
        local_mix, cumulative, block_ends, entering, state_before, read_map, seq_inputs, skip_gain
    )
    combine = combine_map(expert_ids, route_weights, expert_count, capacity)
    summed = jnp.sum(returned.reshape(expert_count, 2, capacity, width), axis=1)
    expert_output = jnp.dot(
        combine,
        summed.reshape(expert_count * capacity, width),
        precision=HIGHEST,
        preferred_element_type=jnp.float32,
    ).astype(jnp.bfloat16)
    return (mixer_output, expert_output)


def solution(mesh):
    devices = mesh.devices
    ctx_size, exp_size = devices.shape
    split = jax.sharding.Mesh(
        devices.reshape(ctx_size // 4, 2, 2, exp_size), ("zh", "zl", "core", "exp")
    )
    return jax.shard_map(
        layer,
        mesh=split,
        in_specs=(
            P(CTX, "exp"),
            P("exp", CTX),
            P(None, CTX),
            P(None, CTX),
            P("exp"),
            P("exp"),
            P("exp", None),
            P("exp", None),
            P("exp", None),
            P("exp", None, CTX),
            P("exp", None, CTX),
            P("exp", None, CTX),
        ),
        out_specs=(P(CTX, "exp"), P("exp", CTX)),
        check_vma=False,
    )
```
